32 devices in a mesh: blk: 16 (over z, y, core), along: 2 (over x).
Axes of the slice: x: 2, y: 2, z: 4, core: 2. Of those that a mesh axis runs over, the one named last changes fastest.
Arguments:
- values: float32 [3, 16, 48, 256], P(None, 'blk', 'along'), may hold values from -6 to 6
- offsets: float32 [3, 16, 48, 256], P(None, 'blk', 'along'), may hold values from 0 to 1
- stiffness: float32 [16, 48, 256], P('blk', 'along'), may hold values from 0.5 to 2
- leaf_basis: float32 [16, 48, 64, 256], P('blk', 'along'), may hold values from -0.375 to 0.375
- transfer: float32 [16, 48, 64, 64], P('blk', 'along'), may hold values from -0.15625 to 0.15625
- slab_transfer_matrices: float32 [16, 2, 64, 64], P('blk', 'along'), may hold values from -0.5 to 0.5
- leaf_coupling_matrices: float32 [16, 30, 64, 64], P('blk'), may hold values from -0.375 to 0.375
- leaf_admissible_mask: int32 [16, 30], P('blk'), may hold values 0 or 1
- top_coupling: float32 [16, 16, 64, 64], P('blk'), may hold values from -0.75 to 0.75
- top_admissible: int32 [16, 16], P('blk'), may hold values 0 or 1
Outputs:
- product: float32 [3, 16, 48, 256], P(None, 'blk', 'along')
The draws below stay inside these ranges and needn't reach their ends.
All inputs are finite; a program needn't handle non-finite values. No bound on the sum of `leaf_admissible_mask` or of `top_admissible` on one device may be relied on, other than what follows from the above.
Results may differ from the reference program's by a relative error of at most 0.0001.
Values sent between devices are 32-bit elements; how exact they have to be, the bound alone decides.
A program may use at most 64 MiB of HBM per device.

```python
import math
import jax
import jax.numpy as jnp
from jax import lax

LEAF = 256
BASIS_RANK = 64
RHS = 3
LD = 24
REACH = 6
SECTOR_COUNT = 16
NAX = 48
SLOT_COUNT = 30


def set_ends(array, key, least, high):
    index_at = [jax.random.randint(jax.random.fold_in(key, axis), (), 0, length) for axis, length in enumerate(array.shape)]
    longest = array.shape.index(max(array.shape))
    next_to = index_at[:longest] + [(index_at[longest] + 1) % array.shape[longest]] + index_at[longest + 1:]
    return array.at[tuple(index_at)].set(least).at[tuple(next_to)].set(high)


def steps_of(rng, shape, cuts, low, high):
    def one(axis_at, parts):
        draws = jax.random.uniform(jax.random.fold_in(jax.random.fold_in(rng, 6), axis_at), (parts,), jnp.float32, low / len(cuts), high / len(cuts))
        return jnp.repeat(jnp.exp(draws), shape[axis_at] // parts).reshape((-1,) + (1,) * (len(shape) - axis_at - 1))

    gain = one(*cuts[0])
    for cut in cuts[1:]:
        gain = gain * one(*cut)
    return gain


def bell_draw(rng, dims, deviation, limit, split=(), held_as=jnp.bfloat16):
    entries = deviation * jax.random.normal(rng, dims, jnp.float32)
    if split:
        entries = entries * steps_of(rng, dims, split, -0.22, 0.18)
    return jnp.clip(entries, -limit, limit).astype(held_as)


def setup_inputs(seed: int = 0) -> dict:
    keys = jax.random.split(jax.random.key(seed), 11)
    values = bell_draw(keys[0], (RHS, SECTOR_COUNT, NAX, LEAF), 1.0, 6.0, ((1, 16), (2, 2)), jnp.float32)
    offsets = jnp.clip(1.0 * jax.random.uniform(keys[1], (3, SECTOR_COUNT, NAX, LEAF), jnp.float32) ** steps_of(keys[1], (3, SECTOR_COUNT, NAX, LEAF), ((1, 16), (2, 2)), -0.2, 0.2), 0.0, 1.0)
    stiffness = jnp.clip(jnp.exp(math.log(2.0) - 1.3862944 * jax.random.uniform(keys[2], (SECTOR_COUNT, NAX, LEAF), jnp.float32) ** steps_of(keys[2], (SECTOR_COUNT, NAX, LEAF), ((0, 16), (1, 2)), -0.2, 0.2)), 0.5, 2.0)
    leaf_basis = bell_draw(keys[3], (SECTOR_COUNT, NAX, BASIS_RANK, LEAF), LEAF ** -0.5, 0.375, ((0, 16), (1, 2)), jnp.float32)
    transfer = bell_draw(keys[4], (SECTOR_COUNT, NAX, BASIS_RANK, BASIS_RANK), (BASIS_RANK * LD) ** -0.5, 0.15625, ((0, 16), (1, 2)), jnp.float32)
    slab_transfer_matrices = bell_draw(keys[5], (SECTOR_COUNT, NAX // LD, BASIS_RANK, BASIS_RANK), (BASIS_RANK * NAX // LD) ** -0.5, 0.5, ((0, 16), (1, 2)), jnp.float32)
    leaf_coupling_matrices = bell_draw(keys[6], (SECTOR_COUNT, SLOT_COUNT, BASIS_RANK, BASIS_RANK), (4 * BASIS_RANK) ** -0.5, 0.375, ((0, 16),), jnp.float32)
    leaf_admissible_mask = set_ends((jax.random.randint(keys[7], (SECTOR_COUNT, SLOT_COUNT), 0, 4) < 3).astype(jnp.int32), jax.random.fold_in(keys[7], 1), 0, 1)
    top_coupling = bell_draw(keys[8], (SECTOR_COUNT, SECTOR_COUNT, BASIS_RANK, BASIS_RANK), BASIS_RANK ** -0.5, 0.75, ((0, 16),), jnp.float32)
    top_admissible = set_ends((jax.random.randint(keys[9], (SECTOR_COUNT, SECTOR_COUNT), 0, 4) < 3).astype(jnp.int32), jax.random.fold_in(keys[9], 1), 0, 1)
    return {"values": values, "offsets": offsets, "stiffness": stiffness, "leaf_basis": leaf_basis, "transfer": transfer, "slab_transfer_matrices": slab_transfer_matrices, "leaf_coupling_matrices": leaf_coupling_matrices, "leaf_admissible_mask": leaf_admissible_mask, "top_coupling": top_coupling, "top_admissible": top_admissible}


SHARPNESS = 2.0
KERNEL_SCALE = 0.125
HIGHEST_ACCURACY = lax.Precision.HIGHEST


def near_field(padded):
    leaves = padded.shape[2] - 2
    center = padded[:, 1:2, 1:1 + leaves]
    result = jnp.zeros((3, 1, leaves, padded.shape[3]), jnp.float32)
    for around in (-1, 0, 1):
        for along_step in (-1, 0, 1):
            source = padded[:, 1 + around:2 + around, 1 + along_step:1 + along_step + leaves]
            gap_around = around + source[0][..., None, :] - center[0][..., :, None]
            gap_along = along_step + source[1][..., None, :] - center[1][..., :, None]
            gap_radial = source[2][..., None, :] - center[2][..., :, None]
            squared = gap_around * gap_around + gap_along * gap_along + gap_radial * gap_radial
            kernel = KERNEL_SCALE * center[3][..., :, None] * source[3][..., None, :] * jnp.exp(-SHARPNESS * squared)
            result = result + jnp.einsum('alij,ralj->rali', kernel, source[4:], precision=HIGHEST_ACCURACY)
    return result


def slot_number(around, along_step, reach):
    block = around - 2 if around > 0 else reach - 1 + (-around - 2)
    return 3 * block + along_step + 1


def reference(values, offsets, stiffness, leaf_basis, transfer, slab_transfer_matrices, leaf_coupling_matrices, leaf_admissible_mask, top_coupling, top_admissible):
    stacked = jnp.concatenate([offsets, stiffness[None], values], 0)
    stacked = jnp.pad(stacked, ((0, 0), (0, 0), (1, 1), (0, 0)))
    stacked = jnp.concatenate([stacked[:, -1:], stacked, stacked[:, :1]], 1)

    def one_sector(sector):
        block = lax.dynamic_slice_in_dim(stacked, sector, 3, 1)
        return near_field(block)[:, 0]

    near = lax.map(one_sector, jnp.arange(SECTOR_COUNT, dtype=jnp.int32))
    near = jnp.transpose(near, (1, 0, 2, 3))

    coefs = jnp.einsum('slki,rsli->rslk', leaf_basis, values, precision=HIGHEST_ACCURACY)
    padded_coefs = jnp.pad(coefs, ((0, 0), (0, 0), (1, 1), (0, 0)))
    far_leaf = jnp.zeros(coefs.shape, jnp.float32)
    offsets_list = list(range(2, REACH + 1)) + [-step for step in range(2, REACH + 1)]
    for around in offsets_list:
        rolled = jnp.roll(padded_coefs, -around, axis=1)
        for along_step in (-1, 0, 1):
            slot = slot_number(around, along_step, REACH)
            partner = rolled[:, :, 1 + along_step:1 + along_step + NAX]
            coupling = leaf_coupling_matrices[:, slot] * leaf_admissible_mask[:, slot].astype(jnp.float32)[:, None, None]
            far_leaf = far_leaf + jnp.einsum('skq,rslq->rslk', coupling, partner, precision=HIGHEST_ACCURACY)

    slabs = NAX // LD
    grouped = coefs.reshape(RHS, SECTOR_COUNT, slabs, LD, BASIS_RANK)
    links = transfer.reshape(SECTOR_COUNT, slabs, LD, BASIS_RANK, BASIS_RANK)
    slab_coefficient_rows = jnp.einsum('splqk,rsplq->rspk', links, grouped, precision=HIGHEST_ACCURACY)
    sector_coefs = jnp.einsum('spqk,rspq->rsk', slab_transfer_matrices, slab_coefficient_rows, precision=HIGHEST_ACCURACY)

    indices = jnp.arange(SECTOR_COUNT, dtype=jnp.int32)
    apart = (indices[None, :] - indices[:, None]) % SECTOR_COUNT
    distant = jnp.logical_and(apart > REACH, apart < SECTOR_COUNT - REACH).astype(jnp.float32)
    allowed = top_admissible.astype(jnp.float32) * distant
    sector_local_coefs = jnp.einsum('stkq,rtq->rsk', top_coupling * allowed[:, :, None, None], sector_coefs, precision=HIGHEST_ACCURACY)

    slab_local_coefs = jnp.einsum('spqk,rsk->rspq', slab_transfer_matrices, sector_local_coefs, precision=HIGHEST_ACCURACY)
    leaf_down = jnp.einsum('splqk,rspk->rsplq', links, slab_local_coefs, precision=HIGHEST_ACCURACY).reshape(RHS, SECTOR_COUNT, NAX, BASIS_RANK)
    leaf_local = far_leaf + leaf_down
    return near + jnp.einsum('slki,rslk->rsli', leaf_basis, leaf_local, precision=HIGHEST_ACCURACY)
```

```python
import functools

import jax
import jax.numpy as jnp
from jax import lax
from jax.experimental import pallas as pl
from jax.experimental.pallas import tpu as pltpu
from jax.sharding import PartitionSpec as P

REACH = 6


SHARPNESS = 2.0
KERNEL_SCALE = 0.125
HIGHEST_ACCURACY = lax.Precision.HIGHEST


LOG2E = 1.4426950408889634


def halves(x):
    high = x.astype(jnp.bfloat16)
    return high, (x - high.astype(jnp.float32)).astype(jnp.bfloat16)


def near_steps(cells_ref, stiff_ref, near_ref, work):
    feature_ref, low_ref, high_ref, weight_ref, point_ref, factor_ref, *tiles = work
    leaves, size = stiff_ref.shape
    slots = cells_ref.shape[2]
    group = 16

    def prepare(a):
        for g in range(slots // group):
            rows = pl.ds(group * g, group)
            y0 = cells_ref[a, 0, rows] + (a - 1.0)
            y1, y2 = cells_ref[a, 1, rows], cells_ref[a, 2, rows]
            norm = (-SHARPNESS * LOG2E) * (y0 * y0 + y1 * y1 + y2 * y2)
            coarse = norm.astype(jnp.bfloat16).astype(jnp.float32)
            stacked = jnp.concatenate([y0, y1, y2, coarse, y0, y1, y2, norm - coarse], 0).T
            feature_ref[a, g] = jnp.concatenate(halves(stacked), 1)
        for k in range(2):
            lanes = pl.ds(128 * k, 128)
            wide = (low_ref, high_ref)[k]
            for g in range(slots // 8):
                for r in range(3):
                    w = cells_ref[a, 3 + r, pl.ds(8 * g, 8), lanes]
                    rounded = w.astype(jnp.bfloat16).astype(jnp.float32)
                    wide[pl.ds(128 * g + r, 8, stride=16)] = rounded
                    wide[pl.ds(128 * g + 8 + r, 8, stride=16)] = w - rounded
            weight_ref[a, :, lanes] = wide[...].astype(jnp.bfloat16)

    def targets():
        low_ref[...] = jnp.zeros_like(low_ref)
        high_ref[...] = jnp.zeros_like(high_ref)
        own = pl.ds(0, leaves)
        x0, x1, x2 = (cells_ref[1, d, own] for d in range(3))
        planes = [x0, x2] + [x1 - (b - 1.0) for b in range(3)]
        for k, z in enumerate(planes):
            z = z * (2 * SHARPNESS * LOG2E)
            rounded = z.astype(jnp.bfloat16).astype(jnp.float32)
            point_ref[2 * k] = rounded
            point_ref[2 * k + 1] = (z - rounded).astype(jnp.bfloat16).astype(jnp.float32)
        across = x0 * x0 + x2 * x2
        for b in range(3):
            z1 = planes[2 + b]
            factor_ref[b] = (
                KERNEL_SCALE * stiff_ref[...] * jnp.exp2((-SHARPNESS * LOG2E) * (across + z1 * z1))
            )

    row = lax.broadcasted_iota(jnp.int32, (group, size), 0)

    def slot_of(leaf):
        return jnp.where(leaf < 0, leaves, jnp.where(leaf >= leaves, leaves + 1, leaf))

    def right_side(t, b):
        slot = slot_of(t + (b - 1))
        chosen = row == lax.rem(slot, group)

        def block(k):
            return jnp.where(chosen, point_ref[k, pl.ds(t, 1)], 0.0).astype(jnp.bfloat16)

        one = jnp.where(chosen, 1.0, 0.0).astype(jnp.bfloat16)
        k = 4 + 2 * b
        blocks = [block(0), block(k), block(2), one, block(1), block(k + 1), block(3), one]
        return slot // group, jnp.concatenate(blocks + blocks, 0)

    def run(sources, first, together):
        count = len(sources)

        def fill(t, i, b, into):
            g, right = right_side(t, b)
            for n, a in enumerate(sources):
                power = jnp.dot(feature_ref[a, g], right, preferred_element_type=jnp.float32)
                high, low = halves(jnp.exp2(power))
                k = (i * 3 + b) * count + n
                into[0][k] = high
                into[1][k] = low

        def use(t, i, b, taken, total):
            slot = slot_of(t + (b - 1))
            got = None
            for n, a in enumerate(sources):
                weight = weight_ref[a, pl.ds(pl.multiple_of(slot * 16, 16), 16)]
                k = (i * 3 + b) * count + n
                for part in taken:
                    term = jnp.dot(weight, part[k], preferred_element_type=jnp.float32)
                    got = term if got is None else got + term
            term = (got[:8] + got[8:]) * factor_ref[b, pl.ds(t, 1)]
            return term if total is None else total + term

        def half(ahead, now, into, taken):
            for i in range(together):
                total = None
                for b in range(3):
                    fill(jnp.minimum(ahead + i, leaves - 1), i, b, into)
                    total = use(now + i, i, b, taken, total)
                for r in range(3):
                    line = total[r : r + 1]
                    at = pl.ds(now + i, 1)
                    near_ref[r, at] = line if first else near_ref[r, at] + line

        even, odd = tiles[:2], tiles[2:]
        for i in range(together):
            for b in range(3):
                fill(i, i, b, even)

        def step(k, carry):
            t = k * 2 * together
            half(t + together, t, odd, even)
            half(t + 2 * together, t + together, even, odd)
            return carry

        lax.fori_loop(0, leaves // (2 * together), step, 0)

    return prepare, targets, run


def far_offsets():
    ahead = list(range(2, REACH + 1))
    return ahead + [-step for step in ahead]


def exchange_kernel(
    cells_ref,
    edges_ref,
    stiff_ref,
    coefs_ref,
    ends_ref,
    share_ref,
    near_ref,
    windows_ref,
    rims_ref,
    shares_ref,
    padded_ref,
    brims_ref,
    send_sem,
    recv_sem,
    share_send_sem,
    share_recv_sem,
    *work,
):
    sectors, slabs = lax.axis_size("blk"), lax.axis_size("along")
    sector, slab = lax.axis_index("blk"), lax.axis_index("along")
    leaves = cells_ref.shape[1]
    slots = padded_ref.shape[2]
    copies = []

    def send(source, target, around, along):
        k = len(copies)
        copy = pltpu.make_async_remote_copy(
            src_ref=source,
            dst_ref=target,
            send_sem=send_sem.at[k],
            recv_sem=recv_sem.at[k],
            device_id={
                "blk": lax.rem(sector + around + sectors, sectors),
                "along": lax.rem(slab + along + slabs, slabs),
            },
            device_id_type=pl.DeviceIdType.MESH,
        )
        copy.start()
        copies.append(copy)

    distant = sectors - 2 * REACH - 1

    def share_copy(k, row, column):
        return pltpu.make_async_remote_copy(
            src_ref=share_ref,
            dst_ref=shares_ref.at[row, column],
            send_sem=share_send_sem.at[k],
            recv_sem=share_recv_sem.at[k // slabs * slabs + column],
            device_id={
                "blk": lax.rem(sector + REACH + 1 + k // slabs, sectors),
                "along": lax.rem(k, slabs),
            },
            device_id_type=pl.DeviceIdType.MESH,
        )

    def share_start(k, carry):
        share_copy(k, sector, slab).start()
        return carry

    def share_wait(k, carry):
        came = lax.rem(sector + sectors - REACH - 1 - k // slabs, sectors)
        share_copy(k, sector, slab).wait_send()
        share_copy(k, came, lax.rem(k, slabs)).wait_recv()
        return carry

    for around in (0, -1, 1):
        send(edges_ref.at[1], brims_ref.at[1 - around, 0], around, 1)
        send(edges_ref.at[0], brims_ref.at[1 - around, 1], around, -1)
    for around in (-1, 1):
        send(cells_ref, padded_ref.at[1 - around, :, pl.ds(0, leaves)], around, 0)
    lax.fori_loop(0, distant * slabs, share_start, 0)
    for q, around in enumerate(far_offsets()):
        send(coefs_ref, windows_ref.at[q], -around, 0)
        send(ends_ref.at[1], rims_ref.at[q, 0], -around, 1)
        send(ends_ref.at[0], rims_ref.at[q, 1], -around, -1)
    prepare, targets, run = near_steps(padded_ref, stiff_ref, near_ref, work)
    padded_ref[1, :, pl.ds(0, leaves)] = cells_ref[...]
    spare = jnp.zeros((slots - leaves, cells_ref.shape[2]), jnp.float32)
    at = lax.broadcasted_iota(jnp.int32, spare.shape, 0)

    def close(a):
        for d in range(6):
            before, after = brims_ref[a, 0, d : d + 1], brims_ref[a, 1, d : d + 1]
            before = jnp.where(slab == 0, 0.0, before)
            after = jnp.where(slab == slabs - 1, 0.0, after)
            padded_ref[a, d, pl.ds(leaves, slots - leaves)] = jnp.where(
                at == 0, before, jnp.where(at == 1, after, spare)
            )

    targets()
    for copy in copies[:2]:
        copy.wait()
    close(1)
    prepare(1)
    run((1,), True, 2)
    for copy in copies[2:8]:
        copy.wait()
    close(0)
    close(2)
    prepare(0)
    prepare(2)
    run((0, 2), False, 2)
    for copy in copies[8:]:
        copy.wait()
    lax.fori_loop(0, distant * slabs, share_wait, 0)

    @pl.when(slab == 0)
    def _():
        rims_ref[:, 0] = jnp.zeros_like(rims_ref[:, 0])

    @pl.when(slab == slabs - 1)
    def _():
        rims_ref[:, 1] = jnp.zeros_like(rims_ref[:, 1])


def exchange(cells, edges, stiffness, coefs, ends, share):
    sectors, slabs = lax.axis_size("blk"), lax.axis_size("along")
    _, leaves, size = cells.shape
    slots = -(-(leaves + 2) // 16) * 16
    far = 2 * (REACH - 1)
    links = 8 + 3 * far
    pairs = (sectors - 2 * REACH - 1) * slabs
    vmem = pl.BlockSpec(memory_space=pltpu.VMEM)
    return pl.pallas_call(
        exchange_kernel,
        out_shape=(
            jax.ShapeDtypeStruct((3, leaves, size), jnp.float32),
            jax.ShapeDtypeStruct((far, *coefs.shape), jnp.float32),
            jax.ShapeDtypeStruct((far, *ends.shape), jnp.float32),
            jax.ShapeDtypeStruct((sectors, slabs, *share.shape), jnp.float32),
        ),
        in_specs=[vmem] * 6,
        out_specs=(vmem,) * 4,
        scratch_shapes=[
            pltpu.VMEM((3, 6, slots, size), jnp.float32),
            pltpu.VMEM((3, 2, 8, size), jnp.float32),
            pltpu.SemaphoreType.DMA((links,)),
            pltpu.SemaphoreType.DMA((links,)),
            pltpu.SemaphoreType.DMA((pairs,)),
            pltpu.SemaphoreType.DMA((pairs,)),
            pltpu.VMEM((3, slots // 16, size, 256), jnp.bfloat16),
            pltpu.VMEM((slots * 16, 128), jnp.float32),
            pltpu.VMEM((slots * 16, 128), jnp.float32),
            pltpu.VMEM((3, slots * 16, size), jnp.bfloat16),
            pltpu.VMEM((10, leaves, size), jnp.float32),
            pltpu.VMEM((3, leaves, size), jnp.float32),
            *[pltpu.VMEM((12, size, size), jnp.bfloat16)] * 4,
        ],
        compiler_params=pltpu.CompilerParams(
            has_side_effects=True, vmem_limit_bytes=40 * 1024 * 1024
        ),
    )(cells, edges, stiffness, coefs, ends, share)


def body(
    values,
    offsets,
    stiffness,
    leaf_basis,
    transfer,
    slab_transfer_matrices,
    leaf_coupling_matrices,
    leaf_admissible_mask,
    top_coupling,
    top_admissible,
):
    cells = jnp.concatenate([offsets - 0.5, stiffness[None] * values], 0)[:, 0]
    edges = jnp.stack([cells[:, 0], cells[:, -1]])
    edges = jnp.pad(edges, ((0, 0), (0, 2), (0, 0)))
    coefs = jnp.einsum("slki,rsli->rslk", leaf_basis, values, precision=HIGHEST_ACCURACY)
    slab_coefficient_rows = jnp.einsum(
        "slqk,rslq->rsk", transfer, coefs, precision=HIGHEST_ACCURACY
    )
    shared_portion = jnp.einsum(
        "oxz,eox->eoz",
        slab_transfer_matrices[:, 0],
        slab_coefficient_rows,
        precision=HIGHEST_ACCURACY,
    )
    by_leaf = coefs[:, 0].transpose(1, 0, 2)
    leaves, count, rank = by_leaf.shape
    width = -(-count * rank // 128) * 128
    lanes = -(-rank // 128) * 128
    flat = by_leaf.reshape(leaves, count * rank)
    ends = jnp.stack([by_leaf[0], by_leaf[-1]])
    near, windows, rims, shares = exchange(
        cells,
        edges,
        stiffness[0],
        jnp.pad(flat, ((0, 0), (0, width - count * rank))),
        jnp.pad(ends, ((0, 0), (0, 8 - count), (0, lanes - rank))),
        jnp.pad(shared_portion[:, 0], ((0, 8 - count), (0, lanes - rank))),
    )
    near = near[:, None]
    far = windows.shape[0]
    windows = windows[:, :, : count * rank].reshape(far, leaves, count, rank)
    rims = rims[:, :, :count, :rank]
    windows = jnp.concatenate([rims[:, :1], windows, rims[:, 1:]], 1)
    partners = jnp.stack([windows[:, b : b + leaves] for b in range(3)], 1)
    coupling = (
        leaf_coupling_matrices[0] * leaf_admissible_mask[0].astype(jnp.float32)[:, None, None]
    ).reshape(far, 3, rank, rank)
    far_leaf = jnp.einsum(
        "qbkz,qblrz->rlk", coupling, partners, precision=HIGHEST_ACCURACY
    )[:, None]
    sectors = lax.axis_size("blk")
    sector = lax.axis_index("blk")
    others = jnp.arange(sectors, dtype=jnp.int32)
    apart = (others - sector) % sectors
    distant = jnp.logical_and(apart > REACH, apart < sectors - REACH)
    allowed = jnp.where(distant, top_admissible[0].astype(jnp.float32), 0.0)
    shares = jnp.where(distant[:, None, None, None], shares, 0.0)
    every_sector = shares.sum(1)[:, :count, :rank].transpose(1, 0, 2)
    sector_local_coefs = jnp.einsum(
        "stkq,rtq->rsk",
        top_coupling * allowed[None, :, None, None],
        every_sector,
        precision=HIGHEST_ACCURACY,
    )
    slab_local_coefs = jnp.einsum(
        "baz,lbz->lba", slab_transfer_matrices[:, 0], sector_local_coefs, precision=HIGHEST_ACCURACY
    )
    leaf_down = jnp.einsum("slqk,rsk->rslq", transfer, slab_local_coefs, precision=HIGHEST_ACCURACY)
    leaf_local = far_leaf + leaf_down
    return near + jnp.einsum("slki,rslk->rsli", leaf_basis, leaf_local, precision=HIGHEST_ACCURACY)


def solution(mesh):
    return jax.shard_map(
        body,
        mesh=mesh,
        in_specs=(
            P(None, "blk", "along", None),
            P(None, "blk", "along", None),
            P("blk", "along", None),
            P("blk", "along", None, None),
            P("blk", "along", None, None),
            P("blk", "along", None, None),
            P("blk", None, None, None),
            P("blk", None),
            P("blk", None, None, None),
            P("blk", None),
        ),
        out_specs=P(None, "blk", "along", None),
        check_vma=False,
    )
```

```python
import jax
import jax.numpy as jnp
from jax import lax
from jax.experimental import pallas as pl
from jax.experimental.pallas import tpu as pltpu
from jax.sharding import PartitionSpec as P

REACH = 6


SHARPNESS = 2.0
KERNEL_SCALE = 0.125


LOG2E = 1.4426950408889634


def halves(x):
    high = x.astype(jnp.bfloat16)
    return high, (x - high.astype(jnp.float32)).astype(jnp.bfloat16)


def near_steps(cells_ref, stiff_ref, near_ref, work):
    feature_ref, low_ref, high_ref, weight_ref, point_ref, factor_ref, *tiles = work
    leaves, size = stiff_ref.shape
    slots = cells_ref.shape[2]
    group = 16

    def prepare(a):
        for g in range(slots // group):
            rows = pl.ds(group * g, group)
            y0 = cells_ref[a, 0, rows] + (a - 1.0)
            y1, y2 = cells_ref[a, 1, rows], cells_ref[a, 2, rows]
            norm = (-SHARPNESS * LOG2E) * (y0 * y0 + y1 * y1 + y2 * y2)
            coarse = norm.astype(jnp.bfloat16).astype(jnp.float32)
            stacked = jnp.concatenate([y0, y1, y2, coarse, y0, y1, y2, norm - coarse], 0).T
            feature_ref[a, g] = jnp.concatenate(halves(stacked), 1)
        for k in range(2):
            lanes = pl.ds(128 * k, 128)
            wide = (low_ref, high_ref)[k]
            for g in range(slots // 8):
                for r in range(3):
                    w = cells_ref[a, 3 + r, pl.ds(8 * g, 8), lanes]
                    rounded = w.astype(jnp.bfloat16).astype(jnp.float32)
                    wide[pl.ds(128 * g + r, 8, stride=16)] = rounded
                    wide[pl.ds(128 * g + 8 + r, 8, stride=16)] = w - rounded
            weight_ref[a, :, lanes] = wide[...].astype(jnp.bfloat16)

    def targets():
        low_ref[...] = jnp.zeros_like(low_ref)
        high_ref[...] = jnp.zeros_like(high_ref)
        own = pl.ds(0, leaves)
        x0, x1, x2 = (cells_ref[1, d, own] for d in range(3))
        planes = [x0, x2] + [x1 - (b - 1.0) for b in range(3)]
        for k, z in enumerate(planes):
            z = z * (2 * SHARPNESS * LOG2E)
            rounded = z.astype(jnp.bfloat16).astype(jnp.float32)
            point_ref[2 * k] = rounded
            point_ref[2 * k + 1] = (z - rounded).astype(jnp.bfloat16).astype(jnp.float32)
        across = x0 * x0 + x2 * x2
        for b in range(3):
            z1 = planes[2 + b]
            factor_ref[b] = (
                KERNEL_SCALE * stiff_ref[...] * jnp.exp2((-SHARPNESS * LOG2E) * (across + z1 * z1))
            )

    row = lax.broadcasted_iota(jnp.int32, (group, size), 0)

    def slot_of(leaf):
        return jnp.where(leaf < 0, leaves, jnp.where(leaf >= leaves, leaves + 1, leaf))

    def right_side(t, b):
        slot = slot_of(t + (b - 1))
        chosen = row == lax.rem(slot, group)

        def block(k):
            return jnp.where(chosen, point_ref[k, pl.ds(t, 1)], 0.0).astype(jnp.bfloat16)

        one = jnp.where(chosen, 1.0, 0.0).astype(jnp.bfloat16)
        k = 4 + 2 * b
        blocks = [block(0), block(k), block(2), one, block(1), block(k + 1), block(3), one]
        return slot // group, jnp.concatenate(blocks + blocks, 0)

    def run(sources, first, together):
        count = len(sources)

        def fill(t, i, b, into):
            g, right = right_side(t, b)
            for n, a in enumerate(sources):
                power = jnp.dot(feature_ref[a, g], right, preferred_element_type=jnp.float32)
                high, low = halves(jnp.exp2(power))
                k = (i * 3 + b) * count + n
                into[0][k] = high
                into[1][k] = low

        def use(t, i, b, taken, total):
            slot = slot_of(t + (b - 1))
            got = None
            for n, a in enumerate(sources):
                weight = weight_ref[a, pl.ds(pl.multiple_of(slot * 16, 16), 16)]
                k = (i * 3 + b) * count + n
                for part in taken:
                    term = jnp.dot(weight, part[k], preferred_element_type=jnp.float32)
                    got = term if got is None else got + term
            term = (got[:8] + got[8:]) * factor_ref[b, pl.ds(t, 1)]
            return term if total is None else total + term

        def half(ahead, now, into, taken):
            for i in range(together):
                total = None
                for b in range(3):
                    fill(jnp.minimum(ahead + i, leaves - 1), i, b, into)
                    total = use(now + i, i, b, taken, total)
                for r in range(3):
                    line = total[r : r + 1]
                    at = pl.ds(now + i, 1)
                    near_ref[r, at] = line if first else near_ref[r, at] + line

        even, odd = tiles[:2], tiles[2:]
        for i in range(together):
            for b in range(3):
                fill(i, i, b, even)

        def step(k, carry):
            t = k * 2 * together
            half(t + together, t, odd, even)
            half(t + 2 * together, t + together, even, odd)
            return carry

        lax.fori_loop(0, leaves // (2 * together), step, 0)

    return prepare, targets, run


def far_offsets():
    ahead = list(range(2, REACH + 1))
    return ahead + [-step for step in ahead]


def stack_halves(x):
    rounded = x.astype(jnp.bfloat16).astype(jnp.float32)
    return jnp.concatenate([rounded, x - rounded], 0).astype(jnp.bfloat16)


def split_product(left, right, transposed):
    dims = (((1,), (1 if transposed else 0,)), ((), ()))
    high, low = halves(right)
    return lax.dot_general(
        left, high, dims, preferred_element_type=jnp.float32
    ) + lax.dot_general(left, low, dims, preferred_element_type=jnp.float32)


def fold(x):
    half = x.shape[0] // 2
    return x[:half] + x[half:]


def exchange_kernel(
    cells_ref,
    edges_ref,
    stiff_ref,
    values_ref,
    basis_ref,
    transfer_ref,
    slab_ref,
    coupling_ref,
    mask_ref,
    top_ref,
    listed_ref,
    out_ref,
    padded_ref,
    brims_ref,
    coefs_ref,
    windows_ref,
    share_ref,
    shares_ref,
    far_ref,
    send_sem,
    recv_sem,
    share_send_sem,
    share_recv_sem,
    *work,
):
    sectors, slabs = lax.axis_size("blk"), lax.axis_size("along")
    sector, slab = lax.axis_index("blk"), lax.axis_index("along")
    leaves = cells_ref.shape[1]
    slots = padded_ref.shape[2]
    count = values_ref.shape[0]
    rank = basis_ref.shape[1]
    copies = []

    def send(source, target, around, along):
        k = len(copies)
        copy = pltpu.make_async_remote_copy(
            src_ref=source,
            dst_ref=target,
            send_sem=send_sem.at[k],
            recv_sem=recv_sem.at[k],
            device_id={
                "blk": lax.rem(sector + around + sectors, sectors),
                "along": lax.rem(slab + along + slabs, slabs),
            },
            device_id_type=pl.DeviceIdType.MESH,
        )
        copy.start()
        copies.append(copy)

    distant = sectors - 2 * REACH - 1

    def share_copy(k, row, column):
        return pltpu.make_async_remote_copy(
            src_ref=share_ref,
            dst_ref=shares_ref.at[row, column],
            send_sem=share_send_sem.at[k],
            recv_sem=share_recv_sem.at[k // slabs * slabs + column],
            device_id={
                "blk": lax.rem(sector + REACH + 1 + k // slabs, sectors),
                "along": lax.rem(k, slabs),
            },
            device_id_type=pl.DeviceIdType.MESH,
        )

    def share_start(k, carry):
        share_copy(k, sector, slab).start()
        return carry

    def share_wait(k, carry):
        came = lax.rem(sector + sectors - REACH - 1 - k // slabs, sectors)
        share_copy(k, sector, slab).wait_send()
        share_copy(k, came, lax.rem(k, slabs)).wait_recv()
        return carry

    for around in (0, -1, 1):
        send(edges_ref.at[1], brims_ref.at[1 - around, 0], around, 1)
        send(edges_ref.at[0], brims_ref.at[1 - around, 1], around, -1)
    for around in (-1, 1):
        send(cells_ref, padded_ref.at[1 - around, :, pl.ds(0, leaves)], around, 0)

    lane = lax.broadcasted_iota(jnp.int32, (rank, 128), 1)

    def up(l, carry):
        columns, sums = carry
        basis, link = basis_ref[l], transfer_ref[l]
        new_columns, new_sums = [], []
        for r in range(count):
            terms = basis * values_ref[r, pl.ds(l, 1)]
            partial = terms[:, :128]
            for k in range(1, terms.shape[1] // 128):
                partial = partial + terms[:, 128 * k : 128 * k + 128]
            column = jnp.sum(partial, axis=1, keepdims=True)
            new_columns.append(jnp.where(lane == l, column, columns[r]))
            new_sums.append(sums[r] + link * column)
        return tuple(new_columns), tuple(new_sums)

    columns, sums = lax.fori_loop(
        0,
        leaves,
        up,
        (
            (jnp.zeros((rank, 128), jnp.float32),) * count,
            (jnp.zeros((rank, rank), jnp.float32),) * count,
        ),
        unroll=2,
    )
    rows = [column.T[:leaves] for column in columns]
    width = coefs_ref.shape[1]
    rows.append(jnp.zeros((leaves, width - count * rank), jnp.float32))
    coefs_ref[...] = jnp.concatenate(rows, 1)
    slab_rows = jnp.concatenate(
        [jnp.sum(x, axis=0, keepdims=True) for x in sums]
        + [jnp.zeros((8 - count, rank), jnp.float32)],
        0,
    )
    portion = fold(split_product(stack_halves(slab_rows), slab_ref[...], False))
    share_ref[...] = jnp.concatenate(
        [portion, jnp.zeros((8, share_ref.shape[1] - rank), jnp.float32)], 1
    )
    offsets = far_offsets()
    for q, around in enumerate(offsets):
        send(coefs_ref, windows_ref.at[q, pl.ds(8, leaves)], -around, 0)
        send(coefs_ref.at[pl.ds(leaves - 8, 8)], windows_ref.at[q, pl.ds(0, 8)], -around, 1)
        send(coefs_ref.at[pl.ds(0, 8)], windows_ref.at[q, pl.ds(leaves + 8, 8)], -around, -1)
    lax.fori_loop(0, distant * slabs, share_start, 0)

    prepare, targets, run = near_steps(padded_ref, stiff_ref, out_ref, work)
    padded_ref[1, :, pl.ds(0, leaves)] = cells_ref[...]
    spare = jnp.zeros((slots - leaves, cells_ref.shape[2]), jnp.float32)
    at = lax.broadcasted_iota(jnp.int32, spare.shape, 0)

    def close(a):
        for d in range(6):
            before, after = brims_ref[a, 0, d : d + 1], brims_ref[a, 1, d : d + 1]
            before = jnp.where(slab == 0, 0.0, before)
            after = jnp.where(slab == slabs - 1, 0.0, after)
            padded_ref[a, d, pl.ds(leaves, slots - leaves)] = jnp.where(
                at == 0, before, jnp.where(at == 1, after, spare)
            )

    targets()
    for copy in copies[:2]:
        copy.wait()
    close(1)
    prepare(1)
    run((1,), True, 2)
    for copy in copies[2:8]:
        copy.wait()
    close(0)
    close(2)
    prepare(0)
    prepare(2)
    run((0, 2), False, 2)
    for copy in copies[8:]:
        copy.wait()
    lax.fori_loop(0, distant * slabs, share_wait, 0)

    @pl.when(slab == 0)
    def _():
        windows_ref[:, pl.ds(0, 8)] = jnp.zeros_like(windows_ref[:, pl.ds(0, 8)])

    @pl.when(slab == slabs - 1)
    def _():
        windows_ref[:, pl.ds(leaves + 8, 8)] = jnp.zeros_like(windows_ref[:, pl.ds(0, 8)])

    total = None
    for q in range(len(offsets)):
        left, right = [], []
        for b in range(3):
            window = windows_ref[q, pl.ds(7 + b, leaves)]
            left.append(
                jnp.concatenate([window[:, rank * r : rank * r + rank] for r in range(count)], 0)
            )
            right.append(coupling_ref[3 * q + b] * mask_ref[0, 3 * q + b].astype(jnp.float32))
        term = split_product(
            stack_halves(jnp.concatenate(left, 1)), jnp.concatenate(right, 1), True
        )
        total = term if total is None else total + term
    far_ref[pl.ds(0, count * leaves)] = jnp.concatenate(
        [fold(total), jnp.zeros((count * leaves, far_ref.shape[1] - rank), jnp.float32)], 1
    )

    def across(k, carry):
        other = lax.rem(sector + REACH + 1 + k, sectors)
        held = shares_ref[other, 0]
        for p in range(1, slabs):
            held = held + shares_ref[other, p]
        block = top_ref[other] * listed_ref[0, other].astype(jnp.float32)
        return carry + fold(split_product(stack_halves(held[:, :rank]), block, True))

    sector_local = lax.fori_loop(0, distant, across, jnp.zeros((8, rank), jnp.float32))
    slab_local = fold(split_product(stack_halves(sector_local), slab_ref[...], True))
    slab_left = stack_halves(slab_local)

    def down(l, carry):
        local = fold(split_product(slab_left, transfer_ref[l], True))
        side = [far_ref[pl.ds(leaves * r + l, 1)][:, :rank] for r in range(count)]
        local = local + jnp.concatenate(side + [jnp.zeros((8 - count, rank), jnp.float32)], 0)
        spread = fold(split_product(stack_halves(local), basis_ref[l], False))
        for r in range(count):
            out_ref[r, pl.ds(l, 1)] = out_ref[r, pl.ds(l, 1)] + spread[r : r + 1]
        return carry

    lax.fori_loop(0, leaves, down, 0, unroll=8 if leaves % 8 == 0 else 1)


def exchange(cells, edges, stiffness, values, basis, transfer, slab, coupling, mask, top, listed):
    sectors, slabs = lax.axis_size("blk"), lax.axis_size("along")
    _, leaves, size = cells.shape
    count, rank = values.shape[0], basis.shape[1]
    width = -(-count * rank // 128) * 128
    lanes = -(-rank // 128) * 128
    slots = -(-(leaves + 2) // 16) * 16
    far = 2 * (REACH - 1)
    links = 8 + 3 * far
    pairs = (sectors - 2 * REACH - 1) * slabs
    vmem = pl.BlockSpec(memory_space=pltpu.VMEM)
    smem = pl.BlockSpec(memory_space=pltpu.SMEM)
    return pl.pallas_call(
        exchange_kernel,
        out_shape=jax.ShapeDtypeStruct((count, leaves, size), jnp.float32),
        in_specs=[vmem] * 8 + [smem, vmem, smem],
        out_specs=vmem,
        scratch_shapes=[
            pltpu.VMEM((3, 6, slots, size), jnp.float32),
            pltpu.VMEM((3, 2, 8, size), jnp.float32),
            pltpu.VMEM((leaves, width), jnp.float32),
            pltpu.VMEM((far, leaves + 16, width), jnp.float32),
            pltpu.VMEM((8, lanes), jnp.float32),
            pltpu.VMEM((sectors, slabs, 8, lanes), jnp.float32),
            pltpu.VMEM((count * leaves, lanes), jnp.float32),
            pltpu.SemaphoreType.DMA((links,)),
            pltpu.SemaphoreType.DMA((links,)),
            pltpu.SemaphoreType.DMA((pairs,)),
            pltpu.SemaphoreType.DMA((pairs,)),
            pltpu.VMEM((3, slots // 16, size, 256), jnp.bfloat16),
            pltpu.VMEM((slots * 16, 128), jnp.float32),
            pltpu.VMEM((slots * 16, 128), jnp.float32),
            pltpu.VMEM((3, slots * 16, size), jnp.bfloat16),
            pltpu.VMEM((10, leaves, size), jnp.float32),
            pltpu.VMEM((3, leaves, size), jnp.float32),
            *[pltpu.VMEM((12, size, size), jnp.bfloat16)] * 4,
        ],
        compiler_params=pltpu.CompilerParams(
            has_side_effects=True, vmem_limit_bytes=40 * 1024 * 1024
        ),
    )(cells, edges, stiffness, values, basis, transfer, slab, coupling, mask, top, listed)


def body(
    values,
    offsets,
    stiffness,
    leaf_basis,
    transfer,
    slab_transfer_matrices,
    leaf_coupling_matrices,
    leaf_admissible_mask,
    top_coupling,
    top_admissible,
):
    cells = jnp.concatenate([offsets - 0.5, stiffness[None] * values], 0)[:, 0]
    edges = jnp.stack([cells[:, 0], cells[:, -1]])
    edges = jnp.pad(edges, ((0, 0), (0, 2), (0, 0)))
    product = exchange(
        cells,
        edges,
        stiffness[0],
        values[:, 0],
        leaf_basis[0],
        transfer[0],
        slab_transfer_matrices[0, 0],
        leaf_coupling_matrices[0],
        leaf_admissible_mask,
        top_coupling[0],
        top_admissible,
    )
    return product[:, None]


def solution(mesh):
    return jax.shard_map(
        body,
        mesh=mesh,
        in_specs=(
            P(None, "blk", "along", None),
            P(None, "blk", "along", None),
            P("blk", "along", None),
            P("blk", "along", None, None),
            P("blk", "along", None, None),
            P("blk", "along", None, None),
            P("blk", None, None, None),
            P("blk", None),
            P("blk", None, None, None),
            P("blk", None),
        ),
        out_specs=P(None, "blk", "along", None),
        check_vma=False,
    )
```

```python
import jax
import jax.numpy as jnp
from jax import lax
from jax.experimental import pallas as pl
from jax.experimental.pallas import tpu as pltpu
from jax.sharding import PartitionSpec as P

REACH = 6


SHARPNESS = 2.0
KERNEL_SCALE = 0.125


LOG2E = 1.4426950408889634


def halves(x):
    high = x.astype(jnp.bfloat16)
    return high, (x - high.astype(jnp.float32)).astype(jnp.bfloat16)


def near_steps(cells_ref, stiff_ref, near_ref, work):
    feature_ref, low_ref, high_ref, weight_ref, point_ref, factor_ref, *tiles = work
    leaves, size = stiff_ref.shape
    slots = cells_ref.shape[2]
    group = 16

    def prepare(a):
        for g in range(slots // group):
            rows = pl.ds(group * g, group)
            y0 = cells_ref[a, 0, rows] + (a - 1.0)
            y1, y2 = cells_ref[a, 1, rows], cells_ref[a, 2, rows]
            norm = (-SHARPNESS * LOG2E) * (y0 * y0 + y1 * y1 + y2 * y2)
            coarse = norm.astype(jnp.bfloat16).astype(jnp.float32)
            stacked = jnp.concatenate([y0, y1, y2, coarse, y0, y1, y2, norm - coarse], 0).T
            feature_ref[a, g] = jnp.concatenate(halves(stacked), 1)
        for k in range(2):
            lanes = pl.ds(128 * k, 128)
            wide = (low_ref, high_ref)[k]
            for g in range(slots // 8):
                for r in range(3):
                    w = cells_ref[a, 3 + r, pl.ds(8 * g, 8), lanes]
                    rounded = w.astype(jnp.bfloat16).astype(jnp.float32)
                    wide[pl.ds(128 * g + r, 8, stride=16)] = rounded
                    wide[pl.ds(128 * g + 8 + r, 8, stride=16)] = w - rounded
            weight_ref[a, :, lanes] = wide[...].astype(jnp.bfloat16)

    def targets():
        low_ref[...] = jnp.zeros_like(low_ref)
        high_ref[...] = jnp.zeros_like(high_ref)
        own = pl.ds(0, leaves)
        x0, x1, x2 = (cells_ref[1, d, own] for d in range(3))
        planes = [x0, x2] + [x1 - (b - 1.0) for b in range(3)]
        for k, z in enumerate(planes):
            z = z * (2 * SHARPNESS * LOG2E)
            rounded = z.astype(jnp.bfloat16).astype(jnp.float32)
            point_ref[2 * k] = rounded
            point_ref[2 * k + 1] = (z - rounded).astype(jnp.bfloat16).astype(jnp.float32)
        across = x0 * x0 + x2 * x2
        for b in range(3):
            z1 = planes[2 + b]
            factor_ref[b] = (
                KERNEL_SCALE * stiff_ref[...] * jnp.exp2((-SHARPNESS * LOG2E) * (across + z1 * z1))
            )

    row = lax.broadcasted_iota(jnp.int32, (group, size), 0)

    def slot_of(leaf):
        return jnp.where(leaf < 0, leaves, jnp.where(leaf >= leaves, leaves + 1, leaf))

    def right_side(t, b):
        slot = slot_of(t + (b - 1))
        chosen = row == lax.rem(slot, group)

        def block(k):
            return jnp.where(chosen, point_ref[k, pl.ds(t, 1)], 0.0).astype(jnp.bfloat16)

        one = jnp.where(chosen, 1.0, 0.0).astype(jnp.bfloat16)
        k = 4 + 2 * b
        blocks = [block(0), block(k), block(2), one, block(1), block(k + 1), block(3), one]
        return slot // group, jnp.concatenate(blocks + blocks, 0)

    def run(sources, first, together):
        count = len(sources)

        def fill(t, i, b, into):
            g, right = right_side(t, b)
            for n, a in enumerate(sources):
                power = jnp.dot(feature_ref[a, g], right, preferred_element_type=jnp.float32)
                high, low = halves(jnp.exp2(power))
                k = (i * 3 + b) * count + n
                into[0][k] = high
                into[1][k] = low

        def use(t, i, b, taken, total):
            slot = slot_of(t + (b - 1))
            got = None
            for n, a in enumerate(sources):
                weight = weight_ref[a, pl.ds(pl.multiple_of(slot * 16, 16), 16)]
                k = (i * 3 + b) * count + n
                for part in taken:
                    term = jnp.dot(weight, part[k], preferred_element_type=jnp.float32)
                    got = term if got is None else got + term
            term = (got[:8] + got[8:]) * factor_ref[b, pl.ds(t, 1)]
            return term if total is None else total + term

        def half(ahead, now, into, taken):
            for i in range(together):
                total = None
                for b in range(3):
                    fill(jnp.minimum(ahead + i, leaves - 1), i, b, into)
                    total = use(now + i, i, b, taken, total)
                for r in range(3):
                    line = total[r : r + 1]
                    at = pl.ds(now + i, 1)
                    near_ref[r, at] = line if first else near_ref[r, at] + line

        even, odd = tiles[:2], tiles[2:]
        for i in range(together):
            for b in range(3):
                fill(i, i, b, even)

        def step(k, carry):
            t = k * 2 * together
            half(t + together, t, odd, even)
            half(t + 2 * together, t + together, even, odd)
            return carry

        lax.fori_loop(0, leaves // (2 * together), step, 0)

    return prepare, targets, run


def far_offsets():
    ahead = list(range(2, REACH + 1))
    return ahead + [-step for step in ahead]


def stack_halves(x):
    rounded = x.astype(jnp.bfloat16).astype(jnp.float32)
    return jnp.concatenate([rounded, x - rounded], 0).astype(jnp.bfloat16)


def split_product(left, right, transposed):
    dims = (((1,), (1 if transposed else 0,)), ((), ()))
    high, low = halves(right)
    return lax.dot_general(
        left, high, dims, preferred_element_type=jnp.float32
    ) + lax.dot_general(left, low, dims, preferred_element_type=jnp.float32)


def fold(x):
    half = x.shape[0] // 2
    return x[:half] + x[half:]


def exchange_kernel(
    *refs,
):
    given, refs = refs[:8], refs[8:]
    mask_ref, listed_ref, out_ref, *refs = refs
    here, refs = refs[:8], refs[8:]
    values_ref, offsets_ref, stiff_ref, basis_ref, transfer_ref = here[:5]
    slab_ref, coupling_ref, top_ref = here[5:]
    exchange_steps(
        given,
        here,
        values_ref,
        offsets_ref,
        stiff_ref,
        basis_ref,
        transfer_ref,
        slab_ref,
        coupling_ref,
        top_ref,
        mask_ref,
        listed_ref,
        out_ref,
        *refs,
    )


def exchange_steps(
    given,
    here,
    values_ref,
    offsets_ref,
    stiff_ref,
    basis_ref,
    transfer_ref,
    slab_ref,
    coupling_ref,
    top_ref,
    mask_ref,
    listed_ref,
    out_ref,
    cells_ref,
    edges_ref,
    padded_ref,
    brims_ref,
    coefs_ref,
    windows_ref,
    share_ref,
    shares_ref,
    far_ref,
    send_sem,
    recv_sem,
    share_send_sem,
    share_recv_sem,
    load_sem,
    *work,
):
    loads = [
        pltpu.make_async_copy(source, target, load_sem.at[k])
        for k, (source, target) in enumerate(zip(given, here))
    ]
    for load in loads:
        load.start()
    sectors, slabs = lax.axis_size("blk"), lax.axis_size("along")
    sector, slab = lax.axis_index("blk"), lax.axis_index("along")
    leaves = cells_ref.shape[1]
    slots = padded_ref.shape[2]
    count = values_ref.shape[0]
    rank = basis_ref.shape[1]
    copies = []

    def send(source, target, around, along):
        k = len(copies)
        copy = pltpu.make_async_remote_copy(
            src_ref=source,
            dst_ref=target,
            send_sem=send_sem.at[k],
            recv_sem=recv_sem.at[k],
            device_id={
                "blk": lax.rem(sector + around + sectors, sectors),
                "along": lax.rem(slab + along + slabs, slabs),
            },
            device_id_type=pl.DeviceIdType.MESH,
        )
        copy.start()
        copies.append(copy)

    distant = sectors - 2 * REACH - 1

    def share_copy(k, row, column):
        return pltpu.make_async_remote_copy(
            src_ref=share_ref,
            dst_ref=shares_ref.at[row, column],
            send_sem=share_send_sem.at[k],
            recv_sem=share_recv_sem.at[k // slabs * slabs + column],
            device_id={
                "blk": lax.rem(sector + REACH + 1 + k // slabs, sectors),
                "along": lax.rem(k, slabs),
            },
            device_id_type=pl.DeviceIdType.MESH,
        )

    def share_start(k, carry):
        share_copy(k, sector, slab).start()
        return carry

    def share_wait(k, carry):
        came = lax.rem(sector + sectors - REACH - 1 - k // slabs, sectors)
        share_copy(k, sector, slab).wait_send()
        share_copy(k, came, lax.rem(k, slabs)).wait_recv()
        return carry

    barrier = pltpu.get_barrier_semaphore()

    def greet(around, along):
        pl.semaphore_signal(
            barrier,
            inc=1,
            device_id={
                "blk": lax.rem(sector + around + sectors, sectors),
                "along": lax.rem(slab + along + slabs, slabs),
            },
            device_id_type=pl.DeviceIdType.MESH,
        )

    greeted = 0
    for around in (0, -1, 1, *far_offsets()):
        for along in (-1, 0, 1):
            if around or along:
                greet(around, along)
                greeted += 1

    def greet_distant(k, carry):
        greet(REACH + 1 + k // slabs, lax.rem(k, slabs))
        return carry

    lax.fori_loop(0, distant * slabs, greet_distant, 0)
    for load in loads[:3]:
        load.wait()
    for d in range(3):
        cells_ref[d] = offsets_ref[d] - 0.5
        cells_ref[3 + d] = stiff_ref[...] * values_ref[d]
    for d in range(6):
        edges_ref[0, pl.ds(d, 1)] = cells_ref[d, pl.ds(0, 1)]
        edges_ref[1, pl.ds(d, 1)] = cells_ref[d, pl.ds(leaves - 1, 1)]
    for k in range(2):
        edges_ref[k, pl.ds(6, 2)] = jnp.zeros((2, edges_ref.shape[2]), jnp.float32)
    pl.semaphore_wait(barrier, greeted + distant * slabs)
    for around in (0, -1, 1):
        send(edges_ref.at[1], brims_ref.at[1 - around, 0], around, 1)
        send(edges_ref.at[0], brims_ref.at[1 - around, 1], around, -1)
    for around in (-1, 1):
        send(cells_ref, padded_ref.at[1 - around, :, pl.ds(0, leaves)], around, 0)

    for load in loads[3:]:
        load.wait()

    lane = lax.broadcasted_iota(jnp.int32, (rank, 128), 1)

    def up(l, carry):
        columns, sums = carry
        basis, link = basis_ref[l], transfer_ref[l]
        new_columns, new_sums = [], []
        for r in range(count):
            terms = basis * values_ref[r, pl.ds(l, 1)]
            partial = terms[:, :128]
            for k in range(1, terms.shape[1] // 128):
                partial = partial + terms[:, 128 * k : 128 * k + 128]
            column = jnp.sum(partial, axis=1, keepdims=True)
            new_columns.append(jnp.where(lane == l, column, columns[r]))
            new_sums.append(sums[r] + link * column)
        return tuple(new_columns), tuple(new_sums)

    columns, sums = lax.fori_loop(
        0,
        leaves,
        up,
        (
            (jnp.zeros((rank, 128), jnp.float32),) * count,
            (jnp.zeros((rank, rank), jnp.float32),) * count,
        ),
        unroll=2,
    )
    rows = [column.T[:leaves] for column in columns]
    width = coefs_ref.shape[1]
    rows.append(jnp.zeros((leaves, width - count * rank), jnp.float32))
    coefs_ref[...] = jnp.concatenate(rows, 1)
    slab_rows = jnp.concatenate(
        [jnp.sum(x, axis=0, keepdims=True) for x in sums]
        + [jnp.zeros((8 - count, rank), jnp.float32)],
        0,
    )
    portion = fold(split_product(stack_halves(slab_rows), slab_ref[...], False))
    share_ref[...] = jnp.concatenate(
        [portion, jnp.zeros((8, share_ref.shape[1] - rank), jnp.float32)], 1
    )
    offsets = far_offsets()
    for q, around in enumerate(offsets):
        send(coefs_ref, windows_ref.at[q, pl.ds(8, leaves)], -around, 0)
        send(coefs_ref.at[pl.ds(leaves - 8, 8)], windows_ref.at[q, pl.ds(0, 8)], -around, 1)
        send(coefs_ref.at[pl.ds(0, 8)], windows_ref.at[q, pl.ds(leaves + 8, 8)], -around, -1)
    lax.fori_loop(0, distant * slabs, share_start, 0)

    prepare, targets, run = near_steps(padded_ref, stiff_ref, out_ref, work)
    padded_ref[1, :, pl.ds(0, leaves)] = cells_ref[...]
    spare = jnp.zeros((slots - leaves, cells_ref.shape[2]), jnp.float32)
    at = lax.broadcasted_iota(jnp.int32, spare.shape, 0)

    def close(a):
        for d in range(6):
            before, after = brims_ref[a, 0, d : d + 1], brims_ref[a, 1, d : d + 1]
            before = jnp.where(slab == 0, 0.0, before)
            after = jnp.where(slab == slabs - 1, 0.0, after)
            padded_ref[a, d, pl.ds(leaves, slots - leaves)] = jnp.where(
                at == 0, before, jnp.where(at == 1, after, spare)
            )

    targets()
    for copy in copies[:2]:
        copy.wait()
    close(1)
    prepare(1)
    run((1,), True, 2)
    for copy in copies[2:8]:
        copy.wait()
    close(0)
    close(2)
    prepare(0)
    prepare(2)
    run((0, 2), False, 2)
    for copy in copies[8:]:
        copy.wait()
    lax.fori_loop(0, distant * slabs, share_wait, 0)

    @pl.when(slab == 0)
    def _():
        windows_ref[:, pl.ds(0, 8)] = jnp.zeros_like(windows_ref[:, pl.ds(0, 8)])

    @pl.when(slab == slabs - 1)
    def _():
        windows_ref[:, pl.ds(leaves + 8, 8)] = jnp.zeros_like(windows_ref[:, pl.ds(0, 8)])

    total = None
    for q in range(len(offsets)):
        left, right = [], []
        for b in range(3):
            window = windows_ref[q, pl.ds(7 + b, leaves)]
            left.append(
                jnp.concatenate([window[:, rank * r : rank * r + rank] for r in range(count)], 0)
            )
            right.append(coupling_ref[3 * q + b] * mask_ref[0, 3 * q + b].astype(jnp.float32))
        term = split_product(
            stack_halves(jnp.concatenate(left, 1)), jnp.concatenate(right, 1), True
        )
        total = term if total is None else total + term
    far_ref[pl.ds(0, count * leaves)] = jnp.concatenate(
        [fold(total), jnp.zeros((count * leaves, far_ref.shape[1] - rank), jnp.float32)], 1
    )

    def across(k, carry):
        other = lax.rem(sector + REACH + 1 + k, sectors)
        held = shares_ref[other, 0]
        for p in range(1, slabs):
            held = held + shares_ref[other, p]
        block = top_ref[other] * listed_ref[0, other].astype(jnp.float32)
        return carry + fold(split_product(stack_halves(held[:, :rank]), block, True))

    sector_local = lax.fori_loop(0, distant, across, jnp.zeros((8, rank), jnp.float32))
    slab_local = fold(split_product(stack_halves(sector_local), slab_ref[...], True))
    slab_left = stack_halves(slab_local)

    def down(l, carry):
        local = fold(split_product(slab_left, transfer_ref[l], True))
        side = [far_ref[pl.ds(leaves * r + l, 1)][:, :rank] for r in range(count)]
        local = local + jnp.concatenate(side + [jnp.zeros((8 - count, rank), jnp.float32)], 0)
        spread = fold(split_product(stack_halves(local), basis_ref[l], False))
        for r in range(count):
            out_ref[r, pl.ds(l, 1)] = out_ref[r, pl.ds(l, 1)] + spread[r : r + 1]
        return carry

    lax.fori_loop(0, leaves, down, 0, unroll=8 if leaves % 8 == 0 else 1)


def exchange(arrays, mask, listed):
    sectors, slabs = lax.axis_size("blk"), lax.axis_size("along")
    count, leaves, size = arrays[0].shape
    rank = arrays[3].shape[1]
    width = -(-count * rank // 128) * 128
    lanes = -(-rank // 128) * 128
    slots = -(-(leaves + 2) // 16) * 16
    far = 2 * (REACH - 1)
    links = 8 + 3 * far
    pairs = (sectors - 2 * REACH - 1) * slabs
    hbm = pl.BlockSpec(memory_space=pltpu.HBM)
    smem = pl.BlockSpec(memory_space=pltpu.SMEM)
    return pl.pallas_call(
        exchange_kernel,
        out_shape=jax.ShapeDtypeStruct((count, leaves, size), jnp.float32),
        in_specs=[hbm] * len(arrays) + [smem] * 2,
        out_specs=pl.BlockSpec(memory_space=pltpu.VMEM),
        scratch_shapes=[
            *[pltpu.VMEM(x.shape, x.dtype) for x in arrays],
            pltpu.VMEM((6, leaves, size), jnp.float32),
            pltpu.VMEM((2, 8, size), jnp.float32),
            pltpu.VMEM((3, 6, slots, size), jnp.float32),
            pltpu.VMEM((3, 2, 8, size), jnp.float32),
            pltpu.VMEM((leaves, width), jnp.float32),
            pltpu.VMEM((far, leaves + 16, width), jnp.float32),
            pltpu.VMEM((8, lanes), jnp.float32),
            pltpu.VMEM((sectors, slabs, 8, lanes), jnp.float32),
            pltpu.VMEM((count * leaves, lanes), jnp.float32),
            pltpu.SemaphoreType.DMA((links,)),
            pltpu.SemaphoreType.DMA((links,)),
            pltpu.SemaphoreType.DMA((pairs,)),
            pltpu.SemaphoreType.DMA((pairs,)),
            pltpu.SemaphoreType.DMA((len(arrays),)),
            pltpu.VMEM((3, slots // 16, size, 256), jnp.bfloat16),
            pltpu.VMEM((slots * 16, 128), jnp.float32),
            pltpu.VMEM((slots * 16, 128), jnp.float32),
            pltpu.VMEM((3, slots * 16, size), jnp.bfloat16),
            pltpu.VMEM((10, leaves, size), jnp.float32),
            pltpu.VMEM((3, leaves, size), jnp.float32),
            *[pltpu.VMEM((12, size, size), jnp.bfloat16)] * 4,
        ],
        compiler_params=pltpu.CompilerParams(
            collective_id=0, has_side_effects=True, vmem_limit_bytes=60 * 1024 * 1024
        ),
    )(*arrays, mask, listed)


def body(
    values,
    offsets,
    stiffness,
    leaf_basis,
    transfer,
    slab_transfer_matrices,
    leaf_coupling_matrices,
    leaf_admissible_mask,
    top_coupling,
    top_admissible,
):
    arrays = (
        values[:, 0],
        offsets[:, 0],
        stiffness[0],
        leaf_basis[0],
        transfer[0],
        slab_transfer_matrices[0, 0],
        leaf_coupling_matrices[0],
        top_coupling[0],
    )
    arrays = tuple(pltpu.with_memory_space_constraint(x, pltpu.HBM) for x in arrays)
    return exchange(arrays, leaf_admissible_mask, top_admissible)[:, None]


def solution(mesh):
    return jax.shard_map(
        body,
        mesh=mesh,
        in_specs=(
            P(None, "blk", "along", None),
            P(None, "blk", "along", None),
            P("blk", "along", None),
            P("blk", "along", None, None),
            P("blk", "along", None, None),
            P("blk", "along", None, None),
            P("blk", None, None, None),
            P("blk", None),
            P("blk", None, None, None),
            P("blk", None),
        ),
        out_specs=P(None, "blk", "along", None),
        check_vma=False,
    )
```

```python
import jax
import jax.numpy as jnp
from jax import lax
from jax.experimental import pallas as pl
from jax.experimental.pallas import tpu as pltpu
from jax.sharding import PartitionSpec as P

REACH = 6


SHARPNESS = 2.0
KERNEL_SCALE = 0.125


LOG2E = 1.4426950408889634


def halves(x):
    high = x.astype(jnp.bfloat16)
    return high, (x - high.astype(jnp.float32)).astype(jnp.bfloat16)


def near_steps(cells_ref, stiff_ref, near_ref, work):
    feature_ref, low_ref, high_ref, weight_ref, point_ref, factor_ref, *tiles = work
    leaves, size = stiff_ref.shape
    slots = cells_ref.shape[2]
    group = 16

    def prepare(a):
        for g in range(slots // group):
            rows = pl.ds(group * g, group)
            y0 = cells_ref[a, 0, rows] + (a - 1.0)
            y1, y2 = cells_ref[a, 1, rows], cells_ref[a, 2, rows]
            norm = (-SHARPNESS * LOG2E) * (y0 * y0 + y1 * y1 + y2 * y2)
            coarse = norm.astype(jnp.bfloat16).astype(jnp.float32)
            stacked = jnp.concatenate([y0, y1, y2, coarse, y0, y1, y2, norm - coarse], 0).T
            feature_ref[a, g] = jnp.concatenate(halves(stacked), 1)
        for k in range(2):
            lanes = pl.ds(128 * k, 128)
            wide = (low_ref, high_ref)[k]
            for g in range(slots // 8):
                for r in range(3):
                    w = cells_ref[a, 3 + r, pl.ds(8 * g, 8), lanes]
                    rounded = w.astype(jnp.bfloat16).astype(jnp.float32)
                    wide[pl.ds(128 * g + r, 8, stride=16)] = rounded
                    wide[pl.ds(128 * g + 8 + r, 8, stride=16)] = w - rounded
            weight_ref[a, :, lanes] = wide[...].astype(jnp.bfloat16)

    def targets():
        low_ref[...] = jnp.zeros_like(low_ref)
        high_ref[...] = jnp.zeros_like(high_ref)
        own = pl.ds(0, leaves)
        x0, x1, x2 = (cells_ref[1, d, own] for d in range(3))
        planes = [x0, x2] + [x1 - (b - 1.0) for b in range(3)]
        for k, z in enumerate(planes):
            z = z * (2 * SHARPNESS * LOG2E)
            rounded = z.astype(jnp.bfloat16).astype(jnp.float32)
            point_ref[2 * k] = rounded
            point_ref[2 * k + 1] = (z - rounded).astype(jnp.bfloat16).astype(jnp.float32)
        across = x0 * x0 + x2 * x2
        for b in range(3):
            z1 = planes[2 + b]
            factor_ref[b] = (
                KERNEL_SCALE * stiff_ref[...] * jnp.exp2((-SHARPNESS * LOG2E) * (across + z1 * z1))
            )

    row = lax.broadcasted_iota(jnp.int32, (group, size), 0)

    def slot_of(leaf):
        return jnp.where(leaf < 0, leaves, jnp.where(leaf >= leaves, leaves + 1, leaf))

    def right_side(t, b):
        slot = slot_of(t + (b - 1))
        chosen = row == lax.rem(slot, group)

        def block(k):
            return jnp.where(chosen, point_ref[k, pl.ds(t, 1)], 0.0).astype(jnp.bfloat16)

        one = jnp.where(chosen, 1.0, 0.0).astype(jnp.bfloat16)
        k = 4 + 2 * b
        blocks = [block(0), block(k), block(2), one, block(1), block(k + 1), block(3), one]
        return slot // group, jnp.concatenate(blocks + blocks, 0)

    def run(sources, first, together):
        count = len(sources)

        def fill(t, i, b, into):
            g, right = right_side(t, b)
            for n, a in enumerate(sources):
                power = jnp.dot(feature_ref[a, g], right, preferred_element_type=jnp.float32)
                high, low = halves(jnp.exp2(power))
                k = (i * 3 + b) * count + n
                into[0][k] = high
                into[1][k] = low

        def use(t, i, b, taken, total):
            slot = slot_of(t + (b - 1))
            got = None
            for n, a in enumerate(sources):
                weight = weight_ref[a, pl.ds(pl.multiple_of(slot * 16, 16), 16)]
                k = (i * 3 + b) * count + n
                for part in taken:
                    term = jnp.dot(weight, part[k], preferred_element_type=jnp.float32)
                    got = term if got is None else got + term
            term = (got[:8] + got[8:]) * factor_ref[b, pl.ds(t, 1)]
            return term if total is None else total + term

        def half(ahead, now, into, taken):
            for i in range(together):
                total = None
                for b in range(3):
                    fill(jnp.minimum(ahead + i, leaves - 1), i, b, into)
                    total = use(now + i, i, b, taken, total)
                for r in range(3):
                    line = total[r : r + 1]
                    at = pl.ds(now + i, 1)
                    near_ref[r, at] = line if first else near_ref[r, at] + line

        even, odd = tiles[:2], tiles[2:]
        for i in range(together):
            for b in range(3):
                fill(i, i, b, even)

        def step(k, carry):
            t = k * 2 * together
            half(t + together, t, odd, even)
            half(t + 2 * together, t + together, even, odd)
            return carry

        lax.fori_loop(0, leaves // (2 * together), step, 0)

    return prepare, targets, run


def far_offsets():
    ahead = list(range(2, REACH + 1))
    return ahead + [-step for step in ahead]


def stack_halves(x):
    rounded = x.astype(jnp.bfloat16).astype(jnp.float32)
    return jnp.concatenate([rounded, x - rounded], 0).astype(jnp.bfloat16)


def split_product(left, right, transposed):
    dims = (((1,), (1 if transposed else 0,)), ((), ()))
    high, low = halves(right)
    return lax.dot_general(
        left, high, dims, preferred_element_type=jnp.float32
    ) + lax.dot_general(left, low, dims, preferred_element_type=jnp.float32)


def fold(x):
    half = x.shape[0] // 2
    return x[:half] + x[half:]


def exchange_kernel(
    *refs,
):
    given, refs = refs[:8], refs[8:]
    mask_ref, listed_ref, out_ref, *refs = refs
    here, refs = refs[:8], refs[8:]
    values_ref, offsets_ref, stiff_ref, basis_ref, transfer_ref = here[:5]
    slab_ref, coupling_ref, top_ref = here[5:]
    exchange_steps(
        given,
        here,
        values_ref,
        offsets_ref,
        stiff_ref,
        basis_ref,
        transfer_ref,
        slab_ref,
        coupling_ref,
        top_ref,
        mask_ref,
        listed_ref,
        out_ref,
        *refs,
    )


def exchange_steps(
    given,
    here,
    values_ref,
    offsets_ref,
    stiff_ref,
    basis_ref,
    transfer_ref,
    slab_ref,
    coupling_ref,
    top_ref,
    mask_ref,
    listed_ref,
    out_ref,
    cells_ref,
    edges_ref,
    padded_ref,
    brims_ref,
    coefs_ref,
    windows_ref,
    share_ref,
    shares_ref,
    far_ref,
    send_sem,
    recv_sem,
    share_send_sem,
    share_recv_sem,
    load_sem,
    *work,
):
    loads = [
        pltpu.make_async_copy(source, target, load_sem.at[k])
        for k, (source, target) in enumerate(zip(given, here))
    ]
    for load in loads:
        load.start()
    sectors, slabs = lax.axis_size("blk"), lax.axis_size("along")
    sector, slab = lax.axis_index("blk"), lax.axis_index("along")
    leaves = cells_ref.shape[1]
    slots = padded_ref.shape[2]
    count = values_ref.shape[0]
    rank = basis_ref.shape[1]
    copies = []

    def send(source, target, around, along):
        k = len(copies)
        copy = pltpu.make_async_remote_copy(
            src_ref=source,
            dst_ref=target,
            send_sem=send_sem.at[k],
            recv_sem=recv_sem.at[k],
            device_id={
                "blk": lax.rem(sector + around + sectors, sectors),
                "along": lax.rem(slab + along + slabs, slabs),
            },
            device_id_type=pl.DeviceIdType.MESH,
        )
        copy.start()
        copies.append(copy)

    distant = sectors - 2 * REACH - 1

    def share_copy(k, row, column):
        return pltpu.make_async_remote_copy(
            src_ref=share_ref,
            dst_ref=shares_ref.at[row, column],
            send_sem=share_send_sem.at[k],
            recv_sem=share_recv_sem.at[k // slabs * slabs + column],
            device_id={
                "blk": lax.rem(sector + REACH + 1 + k // slabs, sectors),
                "along": lax.rem(k, slabs),
            },
            device_id_type=pl.DeviceIdType.MESH,
        )

    def share_start(k, carry):
        share_copy(k, sector, slab).start()
        return carry

    def share_wait(k, carry):
        came = lax.rem(sector + sectors - REACH - 1 - k // slabs, sectors)
        share_copy(k, sector, slab).wait_send()
        share_copy(k, came, lax.rem(k, slabs)).wait_recv()
        return carry

    barrier = pltpu.get_barrier_semaphore()

    def greet(around, along):
        pl.semaphore_signal(
            barrier,
            inc=1,
            device_id={
                "blk": lax.rem(sector + around + sectors, sectors),
                "along": lax.rem(slab + along + slabs, slabs),
            },
            device_id_type=pl.DeviceIdType.MESH,
        )

    greeted = 0
    for around in (0, -1, 1, *far_offsets()):
        for along in (-1, 0, 1):
            if around or along:
                greet(around, along)
                greeted += 1

    def greet_distant(k, carry):
        greet(REACH + 1 + k // slabs, lax.rem(k, slabs))
        return carry

    lax.fori_loop(0, distant * slabs, greet_distant, 0)
    for load in loads[:3]:
        load.wait()
    for d in range(3):
        cells_ref[d] = offsets_ref[d] - 0.5
        cells_ref[3 + d] = stiff_ref[...] * values_ref[d]
    for d in range(6):
        edges_ref[0, pl.ds(d, 1)] = cells_ref[d, pl.ds(0, 1)]
        edges_ref[1, pl.ds(d, 1)] = cells_ref[d, pl.ds(leaves - 1, 1)]
    for k in range(2):
        edges_ref[k, pl.ds(6, 2)] = jnp.zeros((2, edges_ref.shape[2]), jnp.float32)
    for load in loads[3:]:
        load.wait()

    lane = lax.broadcasted_iota(jnp.int32, (rank, 128), 1)

    def up(l, carry):
        columns, sums = carry
        basis, link = basis_ref[l], transfer_ref[l]
        new_columns, new_sums = [], []
        for r in range(count):
            terms = basis * values_ref[r, pl.ds(l, 1)]
            partial = terms[:, :128]
            for k in range(1, terms.shape[1] // 128):
                partial = partial + terms[:, 128 * k : 128 * k + 128]
            column = jnp.sum(partial, axis=1, keepdims=True)
            new_columns.append(jnp.where(lane == l, column, columns[r]))
            new_sums.append(sums[r] + link * column)
        return tuple(new_columns), tuple(new_sums)

    columns, sums = lax.fori_loop(
        0,
        leaves,
        up,
        (
            (jnp.zeros((rank, 128), jnp.float32),) * count,
            (jnp.zeros((rank, rank), jnp.float32),) * count,
        ),
        unroll=2,
    )
    rows = [column.T[:leaves] for column in columns]
    width = coefs_ref.shape[1]
    rows.append(jnp.zeros((leaves, width - count * rank), jnp.float32))
    coefs_ref[...] = jnp.concatenate(rows, 1)
    slab_rows = jnp.concatenate(
        [jnp.sum(x, axis=0, keepdims=True) for x in sums]
        + [jnp.zeros((8 - count, rank), jnp.float32)],
        0,
    )
    portion = fold(split_product(stack_halves(slab_rows), slab_ref[...], False))
    share_ref[...] = jnp.concatenate(
        [portion, jnp.zeros((8, share_ref.shape[1] - rank), jnp.float32)], 1
    )
    prepare, targets, run = near_steps(padded_ref, stiff_ref, out_ref, work)
    padded_ref[1, :, pl.ds(0, leaves)] = cells_ref[...]
    targets()
    pl.semaphore_wait(barrier, greeted + distant * slabs)
    for around in (0, -1, 1):
        send(edges_ref.at[1], brims_ref.at[1 - around, 0], around, 1)
        send(edges_ref.at[0], brims_ref.at[1 - around, 1], around, -1)
    for around in (-1, 1):
        send(cells_ref, padded_ref.at[1 - around, :, pl.ds(0, leaves)], around, 0)
    offsets = far_offsets()
    for q, around in enumerate(offsets):
        send(coefs_ref, windows_ref.at[q, pl.ds(8, leaves)], -around, 0)
        send(coefs_ref.at[pl.ds(leaves - 8, 8)], windows_ref.at[q, pl.ds(0, 8)], -around, 1)
        send(coefs_ref.at[pl.ds(0, 8)], windows_ref.at[q, pl.ds(leaves + 8, 8)], -around, -1)
    lax.fori_loop(0, distant * slabs, share_start, 0)
    spare = jnp.zeros((slots - leaves, cells_ref.shape[2]), jnp.float32)
    at = lax.broadcasted_iota(jnp.int32, spare.shape, 0)

    def close(a):
        for d in range(6):
            before, after = brims_ref[a, 0, d : d + 1], brims_ref[a, 1, d : d + 1]
            before = jnp.where(slab == 0, 0.0, before)
            after = jnp.where(slab == slabs - 1, 0.0, after)
            padded_ref[a, d, pl.ds(leaves, slots - leaves)] = jnp.where(
                at == 0, before, jnp.where(at == 1, after, spare)
            )

    for copy in copies[:2]:
        copy.wait()
    close(1)
    prepare(1)
    run((1,), True, 2)
    for copy in copies[2:8]:
        copy.wait()
    close(0)
    close(2)
    prepare(0)
    prepare(2)
    run((0, 2), False, 2)
    for copy in copies[8:]:
        copy.wait()
    lax.fori_loop(0, distant * slabs, share_wait, 0)

    @pl.when(slab == 0)
    def _():
        windows_ref[:, pl.ds(0, 8)] = jnp.zeros_like(windows_ref[:, pl.ds(0, 8)])

    @pl.when(slab == slabs - 1)
    def _():
        windows_ref[:, pl.ds(leaves + 8, 8)] = jnp.zeros_like(windows_ref[:, pl.ds(0, 8)])

    total = None
    for q in range(len(offsets)):
        left, right = [], []
        for b in range(3):
            window = windows_ref[q, pl.ds(7 + b, leaves)]
            left.append(
                jnp.concatenate([window[:, rank * r : rank * r + rank] for r in range(count)], 0)
            )
            right.append(coupling_ref[3 * q + b] * mask_ref[0, 3 * q + b].astype(jnp.float32))
        term = split_product(
            stack_halves(jnp.concatenate(left, 1)), jnp.concatenate(right, 1), True
        )
        total = term if total is None else total + term
    far_ref[pl.ds(0, count * leaves)] = jnp.concatenate(
        [fold(total), jnp.zeros((count * leaves, far_ref.shape[1] - rank), jnp.float32)], 1
    )

    def facing(k):
        other = lax.rem(sector + REACH + 1 + k, sectors)
        held = shares_ref[other, 0]
        for p in range(1, slabs):
            held = held + shares_ref[other, p]
        return held[:, :rank], top_ref[other] * listed_ref[0, other].astype(jnp.float32)

    def across(k, carry):
        held, block = facing(k)
        return carry + fold(split_product(stack_halves(held), block, True))

    sector_local = jnp.zeros((8, rank), jnp.float32)
    if distant <= 4:
        if distant > 0:
            pairs = [facing(k) for k in range(distant)]
            held, block = (jnp.concatenate(x, 1) for x in zip(*pairs))
            sector_local = fold(split_product(stack_halves(held), block, True))
    else:
        sector_local = lax.fori_loop(0, distant, across, sector_local)
    slab_local = fold(split_product(stack_halves(sector_local), slab_ref[...], True))
    slab_left = stack_halves(slab_local)

    def down(g, carry):
        first = pl.multiple_of(8 * g, 8)
        sides = [far_ref[pl.ds(pl.multiple_of(leaves * r + 8 * g, 8), 8)] for r in range(count)]
        blank = jnp.zeros((8 - count, rank), jnp.float32)
        drops = [fold(split_product(slab_left, transfer_ref[first + n], True)) for n in range(8)]
        lefts = [
            stack_halves(
                drops[n] + jnp.concatenate([x[n : n + 1, :rank] for x in sides] + [blank], 0)
            )
            for n in range(8)
        ]
        spreads = [fold(split_product(lefts[n], basis_ref[first + n], False)) for n in range(8)]
        for r in range(count):
            rows = jnp.concatenate([x[r : r + 1] for x in spreads], 0)
            out_ref[r, pl.ds(first, 8)] = out_ref[r, pl.ds(first, 8)] + rows
        return carry

    lax.fori_loop(0, leaves // 8, down, 0)


def exchange(arrays, mask, listed):
    sectors, slabs = lax.axis_size("blk"), lax.axis_size("along")
    count, leaves, size = arrays[0].shape
    rank = arrays[3].shape[1]
    width = -(-count * rank // 128) * 128
    lanes = -(-rank // 128) * 128
    slots = -(-(leaves + 2) // 16) * 16
    far = 2 * (REACH - 1)
    links = 8 + 3 * far
    pairs = (sectors - 2 * REACH - 1) * slabs
    hbm = pl.BlockSpec(memory_space=pltpu.HBM)
    smem = pl.BlockSpec(memory_space=pltpu.SMEM)
    return pl.pallas_call(
        exchange_kernel,
        out_shape=jax.ShapeDtypeStruct((count, leaves, size), jnp.float32),
        in_specs=[hbm] * len(arrays) + [smem] * 2,
        out_specs=pl.BlockSpec(memory_space=pltpu.VMEM),
        scratch_shapes=[
            *[pltpu.VMEM(x.shape, x.dtype) for x in arrays],
            pltpu.VMEM((6, leaves, size), jnp.float32),
            pltpu.VMEM((2, 8, size), jnp.float32),
            pltpu.VMEM((3, 6, slots, size), jnp.float32),
            pltpu.VMEM((3, 2, 8, size), jnp.float32),
            pltpu.VMEM((leaves, width), jnp.float32),
            pltpu.VMEM((far, leaves + 16, width), jnp.float32),
            pltpu.VMEM((8, lanes), jnp.float32),
            pltpu.VMEM((sectors, slabs, 8, lanes), jnp.float32),
            pltpu.VMEM((count * leaves, lanes), jnp.float32),
            pltpu.SemaphoreType.DMA((links,)),
            pltpu.SemaphoreType.DMA((links,)),
            pltpu.SemaphoreType.DMA((pairs,)),
            pltpu.SemaphoreType.DMA((pairs,)),
            pltpu.SemaphoreType.DMA((len(arrays),)),
            pltpu.VMEM((3, slots // 16, size, 256), jnp.bfloat16),
            pltpu.VMEM((slots * 16, 128), jnp.float32),
            pltpu.VMEM((slots * 16, 128), jnp.float32),
            pltpu.VMEM((3, slots * 16, size), jnp.bfloat16),
            pltpu.VMEM((10, leaves, size), jnp.float32),
            pltpu.VMEM((3, leaves, size), jnp.float32),
            *[pltpu.VMEM((12, size, size), jnp.bfloat16)] * 4,
        ],
        compiler_params=pltpu.CompilerParams(
            collective_id=0, has_side_effects=True, vmem_limit_bytes=40 * 1024 * 1024
        ),
    )(*arrays, mask, listed)


def body(
    values,
    offsets,
    stiffness,
    leaf_basis,
    transfer,
    slab_transfer_matrices,
    leaf_coupling_matrices,
    leaf_admissible_mask,
    top_coupling,
    top_admissible,
):
    arrays = (
        values[:, 0],
        offsets[:, 0],
        stiffness[0],
        leaf_basis[0],
        transfer[0],
        slab_transfer_matrices[0, 0],
        leaf_coupling_matrices[0],
        top_coupling[0],
    )
    arrays = tuple(pltpu.with_memory_space_constraint(x, pltpu.HBM) for x in arrays)
    return exchange(arrays, leaf_admissible_mask, top_admissible)[:, None]


def solution(mesh):
    return jax.shard_map(
        body,
        mesh=mesh,
        in_specs=(
            P(None, "blk", "along", None),
            P(None, "blk", "along", None),
            P("blk", "along", None),
            P("blk", "along", None, None),
            P("blk", "along", None, None),
            P("blk", "along", None, None),
            P("blk", None, None, None),
            P("blk", None),
            P("blk", None, None, None),
            P("blk", None),
        ),
        out_specs=P(None, "blk", "along", None),
        check_vma=False,
    )
```

```python
import jax
import jax.numpy as jnp
from jax import lax
from jax.experimental import pallas as pl
from jax.experimental.pallas import tpu as pltpu
from jax.sharding import PartitionSpec as P

REACH = 6


SHARPNESS = 2.0
KERNEL_SCALE = 0.125


LOG2E = 1.4426950408889634


def halves(x):
    high = x.astype(jnp.bfloat16)
    return high, (x - high.astype(jnp.float32)).astype(jnp.bfloat16)


def near_steps(cells_ref, stiff_ref, near_ref, work):
    feature_ref, low_ref, high_ref, weight_ref, point_ref, factor_ref, *tiles = work
    leaves, size = stiff_ref.shape
    slots = cells_ref.shape[2]
    group = 16

    def prepare(a):
        for g in range(slots // group):
            rows = pl.ds(group * g, group)
            y0 = cells_ref[a, 0, rows] + (a - 1.0)
            y1, y2 = cells_ref[a, 1, rows], cells_ref[a, 2, rows]
            norm = (-SHARPNESS * LOG2E) * (y0 * y0 + y1 * y1 + y2 * y2)
            coarse = norm.astype(jnp.bfloat16).astype(jnp.float32)
            stacked = jnp.concatenate([y0, y1, y2, coarse, y0, y1, y2, norm - coarse], 0).T
            feature_ref[a, g] = jnp.concatenate(halves(stacked), 1)
        for k in range(2):
            lanes = pl.ds(128 * k, 128)
            wide = (low_ref, high_ref)[k]
            for g in range(slots // 8):
                for r in range(3):
                    w = cells_ref[a, 3 + r, pl.ds(8 * g, 8), lanes]
                    rounded = w.astype(jnp.bfloat16).astype(jnp.float32)
                    wide[pl.ds(128 * g + r, 8, stride=16)] = rounded
                    wide[pl.ds(128 * g + 8 + r, 8, stride=16)] = w - rounded
            weight_ref[a, :, lanes] = wide[...].astype(jnp.bfloat16)

    def targets():
        low_ref[...] = jnp.zeros_like(low_ref)
        high_ref[...] = jnp.zeros_like(high_ref)
        own = pl.ds(0, leaves)
        x0, x1, x2 = (cells_ref[1, d, own] for d in range(3))
        planes = [x0, x2] + [x1 - (b - 1.0) for b in range(3)]
        for k, z in enumerate(planes):
            z = z * (2 * SHARPNESS * LOG2E)
            rounded = z.astype(jnp.bfloat16).astype(jnp.float32)
            point_ref[2 * k] = rounded
            point_ref[2 * k + 1] = (z - rounded).astype(jnp.bfloat16).astype(jnp.float32)
        across = x0 * x0 + x2 * x2
        for b in range(3):
            z1 = planes[2 + b]
            factor_ref[b] = (
                KERNEL_SCALE * stiff_ref[...] * jnp.exp2((-SHARPNESS * LOG2E) * (across + z1 * z1))
            )

    row = lax.broadcasted_iota(jnp.int32, (group, size), 0)

    def slot_of(leaf):
        return jnp.where(leaf < 0, leaves, jnp.where(leaf >= leaves, leaves + 1, leaf))

    def right_side(t, b):
        slot = slot_of(t + (b - 1))
        chosen = row == lax.rem(slot, group)

        def block(k):
            return jnp.where(chosen, point_ref[k, pl.ds(t, 1)], 0.0).astype(jnp.bfloat16)

        one = jnp.where(chosen, 1.0, 0.0).astype(jnp.bfloat16)
        k = 4 + 2 * b
        blocks = [block(0), block(k), block(2), one, block(1), block(k + 1), block(3), one]
        return slot // group, jnp.concatenate(blocks + blocks, 0)

    def run(sources, first, together):
        count = len(sources)

        def fill(t, i, b, into):
            g, right = right_side(t, b)
            for n, a in enumerate(sources):
                power = jnp.dot(feature_ref[a, g], right, preferred_element_type=jnp.float32)
                high, low = halves(jnp.exp2(power))
                k = (i * 3 + b) * count + n
                into[0][k] = high
                into[1][k] = low

        def use(t, i, b, taken, total):
            slot = slot_of(t + (b - 1))
            got = None
            for n, a in enumerate(sources):
                weight = weight_ref[a, pl.ds(pl.multiple_of(slot * 16, 16), 16)]
                k = (i * 3 + b) * count + n
                for part in taken:
                    term = jnp.dot(weight, part[k], preferred_element_type=jnp.float32)
                    got = term if got is None else got + term
            term = (got[:8] + got[8:]) * factor_ref[b, pl.ds(t, 1)]
            return term if total is None else total + term

        def half(ahead, now, into, taken):
            for i in range(together):
                total = None
                for b in range(3):
                    fill(jnp.minimum(ahead + i, leaves - 1), i, b, into)
                    total = use(now + i, i, b, taken, total)
                for r in range(3):
                    line = total[r : r + 1]
                    at = pl.ds(now + i, 1)
                    near_ref[r, at] = line if first else near_ref[r, at] + line

        even, odd = tiles[:2], tiles[2:]
        for i in range(together):
            for b in range(3):
                fill(i, i, b, even)

        def step(k, carry):
            t = k * 2 * together
            half(t + together, t, odd, even)
            half(t + 2 * together, t + together, even, odd)
            return carry

        lax.fori_loop(0, leaves // (2 * together), step, 0)

    return prepare, targets, run


def far_offsets():
    ahead = list(range(2, REACH + 1))
    return ahead + [-step for step in ahead]


def stack_halves(x):
    rounded = x.astype(jnp.bfloat16).astype(jnp.float32)
    return jnp.concatenate([rounded, x - rounded], 0).astype(jnp.bfloat16)


def split_product(left, right, transposed):
    dims = (((1,), (1 if transposed else 0,)), ((), ()))
    high, low = halves(right)
    return lax.dot_general(
        left, high, dims, preferred_element_type=jnp.float32
    ) + lax.dot_general(left, low, dims, preferred_element_type=jnp.float32)


def fold(x):
    half = x.shape[0] // 2
    return x[:half] + x[half:]


def exchange_kernel(
    *refs,
):
    given, refs = refs[:10], refs[10:]
    out_ref, *refs = refs
    here, refs = refs[:10], refs[10:]
    values_ref, offsets_ref, stiff_ref, basis_ref, transfer_ref = here[:5]
    slab_ref, coupling_ref, top_ref, mask_ref, listed_ref = here[5:]
    exchange_steps(
        given,
        here,
        values_ref,
        offsets_ref,
        stiff_ref,
        basis_ref,
        transfer_ref,
        slab_ref,
        coupling_ref,
        top_ref,
        mask_ref,
        listed_ref,
        out_ref,
        *refs,
    )


def exchange_steps(
    given,
    here,
    values_ref,
    offsets_ref,
    stiff_ref,
    basis_ref,
    transfer_ref,
    slab_ref,
    coupling_ref,
    top_ref,
    mask_ref,
    listed_ref,
    out_ref,
    cells_ref,
    edges_ref,
    padded_ref,
    brims_ref,
    coefs_ref,
    windows_ref,
    share_ref,
    shares_ref,
    far_ref,
    send_sem,
    recv_sem,
    share_send_sem,
    share_recv_sem,
    load_sem,
    *work,
):
    loads = [
        pltpu.make_async_copy(source, target, load_sem.at[k])
        for k, (source, target) in enumerate(zip(given, here))
    ]
    for load in loads:
        load.start()
    sectors, slabs = lax.axis_size("blk"), lax.axis_size("along")
    sector, slab = lax.axis_index("blk"), lax.axis_index("along")
    leaves = cells_ref.shape[1]
    slots = padded_ref.shape[2]
    count = values_ref.shape[0]
    rank = basis_ref.shape[1]
    copies = []

    def send(source, target, around, along):
        k = len(copies)
        copy = pltpu.make_async_remote_copy(
            src_ref=source,
            dst_ref=target,
            send_sem=send_sem.at[k],
            recv_sem=recv_sem.at[k],
            device_id={
                "blk": lax.rem(sector + around + sectors, sectors),
                "along": lax.rem(slab + along + slabs, slabs),
            },
            device_id_type=pl.DeviceIdType.MESH,
        )
        copy.start()
        copies.append(copy)

    distant = sectors - 2 * REACH - 1

    def share_copy(k, row, column):
        return pltpu.make_async_remote_copy(
            src_ref=share_ref,
            dst_ref=shares_ref.at[row, column],
            send_sem=share_send_sem.at[k],
            recv_sem=share_recv_sem.at[k // slabs * slabs + column],
            device_id={
                "blk": lax.rem(sector + REACH + 1 + k // slabs, sectors),
                "along": lax.rem(k, slabs),
            },
            device_id_type=pl.DeviceIdType.MESH,
        )

    def share_start(k, carry):
        share_copy(k, sector, slab).start()
        return carry

    def share_wait(k, carry):
        came = lax.rem(sector + sectors - REACH - 1 - k // slabs, sectors)
        share_copy(k, sector, slab).wait_send()
        share_copy(k, came, lax.rem(k, slabs)).wait_recv()
        return carry

    barrier = pltpu.get_barrier_semaphore()

    def greet(around, along):
        pl.semaphore_signal(
            barrier,
            inc=1,
            device_id={
                "blk": lax.rem(sector + around + sectors, sectors),
                "along": lax.rem(slab + along + slabs, slabs),
            },
            device_id_type=pl.DeviceIdType.MESH,
        )

    greeted = 0
    for around in (0, -1, 1, *far_offsets()):
        for along in (-1, 0, 1) if slabs > 2 else range(slabs):
            if around or along:
                greet(around, along)
                greeted += 1

    def greet_distant(k, carry):
        greet(REACH + 1 + k // slabs, lax.rem(k, slabs))
        return carry

    lax.fori_loop(0, distant * slabs, greet_distant, 0)
    for load in loads[:3]:
        load.wait()
    for d in range(3):
        cells_ref[d] = offsets_ref[d] - 0.5
        cells_ref[3 + d] = stiff_ref[...] * values_ref[d]
    for d in range(6):
        edges_ref[0, pl.ds(d, 1)] = cells_ref[d, pl.ds(0, 1)]
        edges_ref[1, pl.ds(d, 1)] = cells_ref[d, pl.ds(leaves - 1, 1)]
    for k in range(2):
        edges_ref[k, pl.ds(6, 2)] = jnp.zeros((2, edges_ref.shape[2]), jnp.float32)
    for load in loads[3:]:
        load.wait()

    lane = lax.broadcasted_iota(jnp.int32, (rank, 128), 1)

    def up(l, carry):
        columns, sums = carry
        basis, link = basis_ref[l], transfer_ref[l]
        new_columns, new_sums = [], []
        for r in range(count):
            terms = basis * values_ref[r, pl.ds(l, 1)]
            partial = terms[:, :128]
            for k in range(1, terms.shape[1] // 128):
                partial = partial + terms[:, 128 * k : 128 * k + 128]
            column = jnp.sum(partial, axis=1, keepdims=True)
            new_columns.append(jnp.where(lane == l, column, columns[r]))
            new_sums.append(sums[r] + link * column)
        return tuple(new_columns), tuple(new_sums)

    columns, sums = lax.fori_loop(
        0,
        leaves,
        up,
        (
            (jnp.zeros((rank, 128), jnp.float32),) * count,
            (jnp.zeros((rank, rank), jnp.float32),) * count,
        ),
        unroll=2,
    )
    rows = [column.T[:leaves] for column in columns]
    width = coefs_ref.shape[1]
    rows.append(jnp.zeros((leaves, width - count * rank), jnp.float32))
    coefs_ref[...] = jnp.concatenate(rows, 1)
    slab_rows = jnp.concatenate(
        [jnp.sum(x, axis=0, keepdims=True) for x in sums]
        + [jnp.zeros((8 - count, rank), jnp.float32)],
        0,
    )
    portion = fold(split_product(stack_halves(slab_rows), slab_ref[...], False))
    share_ref[...] = jnp.concatenate(
        [portion, jnp.zeros((8, share_ref.shape[1] - rank), jnp.float32)], 1
    )
    prepare, targets, run = near_steps(padded_ref, stiff_ref, out_ref, work)
    padded_ref[1, :, pl.ds(0, leaves)] = cells_ref[...]
    targets()
    pl.semaphore_wait(barrier, greeted + distant * slabs)
    for around in (0, -1, 1):
        send(edges_ref.at[1], brims_ref.at[1 - around, 0], around, 1)
        send(edges_ref.at[0], brims_ref.at[1 - around, 1], around, -1)
    for around in (-1, 1):
        send(cells_ref, padded_ref.at[1 - around, :, pl.ds(0, leaves)], around, 0)
    spare = jnp.zeros((slots - leaves, cells_ref.shape[2]), jnp.float32)
    at = lax.broadcasted_iota(jnp.int32, spare.shape, 0)

    def close(a):
        for d in range(6):
            before, after = brims_ref[a, 0, d : d + 1], brims_ref[a, 1, d : d + 1]
            before = jnp.where(slab == 0, 0.0, before)
            after = jnp.where(slab == slabs - 1, 0.0, after)
            padded_ref[a, d, pl.ds(leaves, slots - leaves)] = jnp.where(
                at == 0, before, jnp.where(at == 1, after, spare)
            )

    for copy in copies[:2]:
        copy.wait()
    close(1)
    prepare(1)
    run((1,), True, 2)
    offsets = far_offsets()
    for q, around in enumerate(offsets):
        send(coefs_ref, windows_ref.at[q, pl.ds(8, leaves)], -around, 0)
        send(coefs_ref.at[pl.ds(leaves - 8, 8)], windows_ref.at[q, pl.ds(0, 8)], -around, 1)
        send(coefs_ref.at[pl.ds(0, 8)], windows_ref.at[q, pl.ds(leaves + 8, 8)], -around, -1)
    lax.fori_loop(0, distant * slabs, share_start, 0)
    for copy in copies[2:8]:
        copy.wait()
    close(0)
    close(2)
    prepare(0)
    prepare(2)
    run((0, 2), False, 2)
    for copy in copies[8:]:
        copy.wait()
    lax.fori_loop(0, distant * slabs, share_wait, 0)

    @pl.when(slab == 0)
    def _():
        windows_ref[:, pl.ds(0, 8)] = jnp.zeros_like(windows_ref[:, pl.ds(0, 8)])

    @pl.when(slab == slabs - 1)
    def _():
        windows_ref[:, pl.ds(leaves + 8, 8)] = jnp.zeros_like(windows_ref[:, pl.ds(0, 8)])

    total = None
    for q in range(len(offsets)):
        left, right = [], []
        for b in range(3):
            window = windows_ref[q, pl.ds(7 + b, leaves)]
            left.append(
                jnp.concatenate([window[:, rank * r : rank * r + rank] for r in range(count)], 0)
            )
            right.append(coupling_ref[3 * q + b] * mask_ref[0, 3 * q + b].astype(jnp.float32))
        term = split_product(
            stack_halves(jnp.concatenate(left, 1)), jnp.concatenate(right, 1), True
        )
        total = term if total is None else total + term
    far_ref[pl.ds(0, count * leaves)] = jnp.concatenate(
        [fold(total), jnp.zeros((count * leaves, far_ref.shape[1] - rank), jnp.float32)], 1
    )

    def facing(k):
        other = lax.rem(sector + REACH + 1 + k, sectors)
        held = shares_ref[other, 0]
        for p in range(1, slabs):
            held = held + shares_ref[other, p]
        return held[:, :rank], top_ref[other] * listed_ref[0, other].astype(jnp.float32)

    def across(k, carry):
        held, block = facing(k)
        return carry + fold(split_product(stack_halves(held), block, True))

    sector_local = jnp.zeros((8, rank), jnp.float32)
    if distant <= 4:
        if distant > 0:
            pairs = [facing(k) for k in range(distant)]
            held, block = (jnp.concatenate(x, 1) for x in zip(*pairs))
            sector_local = fold(split_product(stack_halves(held), block, True))
    else:
        sector_local = lax.fori_loop(0, distant, across, sector_local)
    slab_local = fold(split_product(stack_halves(sector_local), slab_ref[...], True))
    slab_left = stack_halves(slab_local)

    def down(g, carry):
        first = pl.multiple_of(8 * g, 8)
        sides = [far_ref[pl.ds(pl.multiple_of(leaves * r + 8 * g, 8), 8)] for r in range(count)]
        blank = jnp.zeros((8 - count, rank), jnp.float32)
        drops = [fold(split_product(slab_left, transfer_ref[first + n], True)) for n in range(8)]
        lefts = [
            stack_halves(
                drops[n] + jnp.concatenate([x[n : n + 1, :rank] for x in sides] + [blank], 0)
            )
            for n in range(8)
        ]
        spreads = [fold(split_product(lefts[n], basis_ref[first + n], False)) for n in range(8)]
        for r in range(count):
            rows = jnp.concatenate([x[r : r + 1] for x in spreads], 0)
            out_ref[r, pl.ds(first, 8)] = out_ref[r, pl.ds(first, 8)] + rows
        return carry

    lax.fori_loop(0, leaves // 8, down, 0)


def exchange(arrays):
    sectors, slabs = lax.axis_size("blk"), lax.axis_size("along")
    count, leaves, size = arrays[0].shape
    rank = arrays[3].shape[1]
    width = -(-count * rank // 128) * 128
    lanes = -(-rank // 128) * 128
    slots = -(-(leaves + 2) // 16) * 16
    far = 2 * (REACH - 1)
    links = 8 + 3 * far
    pairs = (sectors - 2 * REACH - 1) * slabs
    hbm = pl.BlockSpec(memory_space=pltpu.HBM)
    return pl.pallas_call(
        exchange_kernel,
        out_shape=jax.ShapeDtypeStruct((count, leaves, size), jnp.float32),
        in_specs=[hbm] * len(arrays),
        out_specs=pl.BlockSpec(memory_space=pltpu.VMEM),
        scratch_shapes=[
            *[pltpu.VMEM(x.shape, x.dtype) for x in arrays[:8]],
            *[pltpu.SMEM(x.shape, x.dtype) for x in arrays[8:]],
            pltpu.VMEM((6, leaves, size), jnp.float32),
            pltpu.VMEM((2, 8, size), jnp.float32),
            pltpu.VMEM((3, 6, slots, size), jnp.float32),
            pltpu.VMEM((3, 2, 8, size), jnp.float32),
            pltpu.VMEM((leaves, width), jnp.float32),
            pltpu.VMEM((far, leaves + 16, width), jnp.float32),
            pltpu.VMEM((8, lanes), jnp.float32),
            pltpu.VMEM((sectors, slabs, 8, lanes), jnp.float32),
            pltpu.VMEM((count * leaves, lanes), jnp.float32),
            pltpu.SemaphoreType.DMA((links,)),
            pltpu.SemaphoreType.DMA((links,)),
            pltpu.SemaphoreType.DMA((pairs,)),
            pltpu.SemaphoreType.DMA((pairs,)),
            pltpu.SemaphoreType.DMA((len(arrays),)),
            pltpu.VMEM((3, slots // 16, size, 256), jnp.bfloat16),
            pltpu.VMEM((slots * 16, 128), jnp.float32),
            pltpu.VMEM((slots * 16, 128), jnp.float32),
            pltpu.VMEM((3, slots * 16, size), jnp.bfloat16),
            pltpu.VMEM((10, leaves, size), jnp.float32),
            pltpu.VMEM((3, leaves, size), jnp.float32),
            *[pltpu.VMEM((12, size, size), jnp.bfloat16)] * 4,
        ],
        compiler_params=pltpu.CompilerParams(
            collective_id=0, has_side_effects=True, vmem_limit_bytes=40 * 1024 * 1024
        ),
    )(*arrays)


def body(
    values,
    offsets,
    stiffness,
    leaf_basis,
    transfer,
    slab_transfer_matrices,
    leaf_coupling_matrices,
    leaf_admissible_mask,
    top_coupling,
    top_admissible,
):
    arrays = (
        values[:, 0],
        offsets[:, 0],
        stiffness[0],
        leaf_basis[0],
        transfer[0],
        slab_transfer_matrices[0, 0],
        leaf_coupling_matrices[0],
        top_coupling[0],
        leaf_admissible_mask,
        top_admissible,
    )
    arrays = tuple(pltpu.with_memory_space_constraint(x, pltpu.HBM) for x in arrays)
    return exchange(arrays)[:, None]


def solution(mesh):
    return jax.shard_map(
        body,
        mesh=mesh,
        in_specs=(
            P(None, "blk", "along", None),
            P(None, "blk", "along", None),
            P("blk", "along", None),
            P("blk", "along", None, None),
            P("blk", "along", None, None),
            P("blk", "along", None, None),
            P("blk", None, None, None),
            P("blk", None),
            P("blk", None, None, None),
            P("blk", None),
        ),
        out_specs=P(None, "blk", "along", None),
        check_vma=False,
    )
```

```python
import jax
import jax.numpy as jnp
from jax import lax
from jax.experimental import pallas as pl
from jax.experimental.pallas import tpu as pltpu
from jax.sharding import PartitionSpec as P

REACH = 6


SHARPNESS = 2.0
KERNEL_SCALE = 0.125


LOG2E = 1.4426950408889634


def halves(x):
    high = x.astype(jnp.bfloat16)
    return high, (x - high.astype(jnp.float32)).astype(jnp.bfloat16)


def near_steps(cells_ref, stiff_ref, near_ref, work):
    feature_ref, low_ref, high_ref, weight_ref, point_ref, factor_ref, *tiles = work
    leaves, size = stiff_ref.shape
    slots = cells_ref.shape[2]
    group = 16

    def prepare(a):
        for g in range(slots // group):
            rows = pl.ds(group * g, group)
            y0 = cells_ref[a, 0, rows] + (a - 1.0)
            y1, y2 = cells_ref[a, 1, rows], cells_ref[a, 2, rows]
            norm = (-SHARPNESS * LOG2E) * (y0 * y0 + y1 * y1 + y2 * y2)
            coarse = norm.astype(jnp.bfloat16).astype(jnp.float32)
            stacked = jnp.concatenate([y0, y1, y2, coarse, y0, y1, y2, norm - coarse], 0).T
            feature_ref[a, g] = jnp.concatenate(halves(stacked), 1)
        for k in range(2):
            lanes = pl.ds(128 * k, 128)
            wide = (low_ref, high_ref)[k]
            for g in range(slots // 8):
                for r in range(3):
                    w = cells_ref[a, 3 + r, pl.ds(8 * g, 8), lanes]
                    rounded = w.astype(jnp.bfloat16).astype(jnp.float32)
                    wide[pl.ds(128 * g + r, 8, stride=16)] = rounded
                    wide[pl.ds(128 * g + 8 + r, 8, stride=16)] = w - rounded
            weight_ref[a, :, lanes] = wide[...].astype(jnp.bfloat16)

    def targets():
        low_ref[...] = jnp.zeros_like(low_ref)
        high_ref[...] = jnp.zeros_like(high_ref)
        own = pl.ds(0, leaves)
        x0, x1, x2 = (cells_ref[1, d, own] for d in range(3))
        planes = [x0, x2] + [x1 - (b - 1.0) for b in range(3)]
        for k, z in enumerate(planes):
            z = z * (2 * SHARPNESS * LOG2E)
            rounded = z.astype(jnp.bfloat16).astype(jnp.float32)
            point_ref[2 * k] = rounded
            point_ref[2 * k + 1] = (z - rounded).astype(jnp.bfloat16).astype(jnp.float32)
        across = x0 * x0 + x2 * x2
        for b in range(3):
            z1 = planes[2 + b]
            factor_ref[b] = (
                KERNEL_SCALE * stiff_ref[...] * jnp.exp2((-SHARPNESS * LOG2E) * (across + z1 * z1))
            )

    row = lax.broadcasted_iota(jnp.int32, (group, size), 0)

    def slot_of(leaf):
        return jnp.where(leaf < 0, leaves, jnp.where(leaf >= leaves, leaves + 1, leaf))

    def right_side(t, b):
        slot = slot_of(t + (b - 1))
        chosen = row == lax.rem(slot, group)

        def block(k):
            return jnp.where(chosen, point_ref[k, pl.ds(t, 1)], 0.0).astype(jnp.bfloat16)

        one = jnp.where(chosen, 1.0, 0.0).astype(jnp.bfloat16)
        k = 4 + 2 * b
        blocks = [block(0), block(k), block(2), one, block(1), block(k + 1), block(3), one]
        return slot // group, jnp.concatenate(blocks + blocks, 0)

    def run(sources, first, together):
        count = len(sources)

        def fill(t, i, b, into):
            g, right = right_side(t, b)
            for n, a in enumerate(sources):
                power = jnp.dot(feature_ref[a, g], right, preferred_element_type=jnp.float32)
                high, low = halves(jnp.exp2(power))
                k = (i * 3 + b) * count + n
                into[0][k] = high
                into[1][k] = low

        def use(t, i, b, taken, total):
            slot = slot_of(t + (b - 1))
            got = None
            for n, a in enumerate(sources):
                weight = weight_ref[a, pl.ds(pl.multiple_of(slot * 16, 16), 16)]
                k = (i * 3 + b) * count + n
                for part in taken:
                    term = jnp.dot(weight, part[k], preferred_element_type=jnp.float32)
                    got = term if got is None else got + term
            term = (got[:8] + got[8:]) * factor_ref[b, pl.ds(t, 1)]
            return term if total is None else total + term

        def half(ahead, now, into, taken):
            for i in range(together):
                total = None
                for b in range(3):
                    fill(jnp.minimum(ahead + i, leaves - 1), i, b, into)
                    total = use(now + i, i, b, taken, total)
                for r in range(3):
                    line = total[r : r + 1]
                    at = pl.ds(now + i, 1)
                    near_ref[r, at] = line if first else near_ref[r, at] + line

        even, odd = tiles[:2], tiles[2:]
        for i in range(together):
            for b in range(3):
                fill(i, i, b, even)

        def step(k, carry):
            t = k * 2 * together
            half(t + together, t, odd, even)
            half(t + 2 * together, t + together, even, odd)
            return carry

        lax.fori_loop(0, leaves // (2 * together), step, 0)

    return prepare, targets, run


def far_offsets():
    ahead = list(range(2, REACH + 1))
    return ahead + [-step for step in ahead]


def stack_halves(x):
    rounded = x.astype(jnp.bfloat16).astype(jnp.float32)
    return jnp.concatenate([rounded, x - rounded], 0).astype(jnp.bfloat16)


def split_product(left, right, transposed):
    dims = (((1,), (1 if transposed else 0,)), ((), ()))
    high, low = halves(right)
    return lax.dot_general(
        left, high, dims, preferred_element_type=jnp.float32
    ) + lax.dot_general(left, low, dims, preferred_element_type=jnp.float32)


def fold(x):
    half = x.shape[0] // 2
    return x[:half] + x[half:]


def exchange_kernel(
    *refs,
):
    given, refs = refs[:10], refs[10:]
    out_ref, *refs = refs
    here, refs = refs[:10], refs[10:]
    values_ref, offsets_ref, stiff_ref, basis_ref, transfer_ref = here[:5]
    slab_ref, coupling_ref, top_ref, mask_ref, listed_ref = here[5:]
    exchange_steps(
        given,
        here,
        values_ref,
        offsets_ref,
        stiff_ref,
        basis_ref,
        transfer_ref,
        slab_ref,
        coupling_ref,
        top_ref,
        mask_ref,
        listed_ref,
        out_ref,
        *refs,
    )


def exchange_steps(
    given,
    here,
    values_ref,
    offsets_ref,
    stiff_ref,
    basis_ref,
    transfer_ref,
    slab_ref,
    coupling_ref,
    top_ref,
    mask_ref,
    listed_ref,
    out_ref,
    cells_ref,
    edges_ref,
    padded_ref,
    brims_ref,
    coefs_ref,
    windows_ref,
    share_ref,
    shares_ref,
    far_ref,
    send_sem,
    recv_sem,
    share_send_sem,
    share_recv_sem,
    load_sem,
    *work,
):
    loads = [
        pltpu.make_async_copy(source, target, load_sem.at[k])
        for k, (source, target) in enumerate(zip(given, here))
    ]
    for load in loads:
        load.start()
    sectors, slabs = lax.axis_size("blk"), lax.axis_size("along")
    sector, slab = lax.axis_index("blk"), lax.axis_index("along")
    leaves = cells_ref.shape[1]
    slots = padded_ref.shape[2]
    count = values_ref.shape[0]
    rank = basis_ref.shape[1]
    copies = []

    def send(source, target, around, along):
        k = len(copies)
        copy = pltpu.make_async_remote_copy(
            src_ref=source,
            dst_ref=target,
            send_sem=send_sem.at[k],
            recv_sem=recv_sem.at[k],
            device_id={
                "blk": lax.rem(sector + around + sectors, sectors),
                "along": lax.rem(slab + along + slabs, slabs),
            },
            device_id_type=pl.DeviceIdType.MESH,
        )
        copy.start()
        copies.append(copy)

    distant = sectors - 2 * REACH - 1

    def share_copy(k, row, column):
        return pltpu.make_async_remote_copy(
            src_ref=share_ref,
            dst_ref=shares_ref.at[row, column],
            send_sem=share_send_sem.at[k],
            recv_sem=share_recv_sem.at[k // slabs * slabs + column],
            device_id={
                "blk": lax.rem(sector + REACH + 1 + k // slabs, sectors),
                "along": lax.rem(k, slabs),
            },
            device_id_type=pl.DeviceIdType.MESH,
        )

    def share_start(k, carry):
        share_copy(k, sector, slab).start()
        return carry

    def share_wait(k, carry):
        came = lax.rem(sector + sectors - REACH - 1 - k // slabs, sectors)
        share_copy(k, sector, slab).wait_send()
        share_copy(k, came, lax.rem(k, slabs)).wait_recv()
        return carry

    barrier = pltpu.get_barrier_semaphore()

    def greet(around, along):
        pl.semaphore_signal(
            barrier,
            inc=1,
            device_id={
                "blk": lax.rem(sector + around + sectors, sectors),
                "along": lax.rem(slab + along + slabs, slabs),
            },
            device_id_type=pl.DeviceIdType.MESH,
        )

    greeted = 0
    for around in (0, -1, 1, *far_offsets()):
        for along in (-1, 0, 1) if slabs > 2 else range(slabs):
            if around or along:
                greet(around, along)
                greeted += 1

    def greet_distant(k, carry):
        greet(REACH + 1 + k // slabs, lax.rem(k, slabs))
        return carry

    lax.fori_loop(0, distant * slabs, greet_distant, 0)
    for load in loads[:3]:
        load.wait()
    for d in range(3):
        cells_ref[d] = offsets_ref[d] - 0.5
        cells_ref[3 + d] = stiff_ref[...] * values_ref[d]
    for d in range(6):
        edges_ref[0, pl.ds(d, 1)] = cells_ref[d, pl.ds(0, 1)]
        edges_ref[1, pl.ds(d, 1)] = cells_ref[d, pl.ds(leaves - 1, 1)]
    for k in range(2):
        edges_ref[k, pl.ds(6, 2)] = jnp.zeros((2, edges_ref.shape[2]), jnp.float32)
    for load in loads[3:]:
        load.wait()

    lane = lax.broadcasted_iota(jnp.int32, (rank, 128), 1)

    def up(l, carry):
        columns, sums = carry
        basis, link = basis_ref[l], transfer_ref[l]
        new_columns, new_sums = [], []
        for r in range(count):
            terms = basis * values_ref[r, pl.ds(l, 1)]
            partial = terms[:, :128]
            for k in range(1, terms.shape[1] // 128):
                partial = partial + terms[:, 128 * k : 128 * k + 128]
            column = jnp.sum(partial, axis=1, keepdims=True)
            new_columns.append(jnp.where(lane == l, column, columns[r]))
            new_sums.append(sums[r] + link * column)
        return tuple(new_columns), tuple(new_sums)

    columns, sums = lax.fori_loop(
        0,
        leaves,
        up,
        (
            (jnp.zeros((rank, 128), jnp.float32),) * count,
            (jnp.zeros((rank, rank), jnp.float32),) * count,
        ),
        unroll=2,
    )
    rows = [column.T[:leaves] for column in columns]
    width = coefs_ref.shape[1]
    rows.append(jnp.zeros((leaves, width - count * rank), jnp.float32))
    coefs_ref[...] = jnp.concatenate(rows, 1)
    slab_rows = jnp.concatenate(
        [jnp.sum(x, axis=0, keepdims=True) for x in sums]
        + [jnp.zeros((8 - count, rank), jnp.float32)],
        0,
    )
    portion = fold(split_product(stack_halves(slab_rows), slab_ref[...], False))
    share_ref[...] = jnp.concatenate(
        [portion, jnp.zeros((8, share_ref.shape[1] - rank), jnp.float32)], 1
    )
    prepare, targets, run = near_steps(padded_ref, stiff_ref, out_ref, work)
    padded_ref[1, :, pl.ds(0, leaves)] = cells_ref[...]
    targets()
    pl.semaphore_wait(barrier, greeted + distant * slabs)
    for around in (0, -1, 1):
        send(edges_ref.at[1], brims_ref.at[1 - around, 0], around, 1)
        send(edges_ref.at[0], brims_ref.at[1 - around, 1], around, -1)
    for around in (-1, 1):
        send(cells_ref, padded_ref.at[1 - around, :, pl.ds(0, leaves)], around, 0)
    spare = jnp.zeros((slots - leaves, cells_ref.shape[2]), jnp.float32)
    at = lax.broadcasted_iota(jnp.int32, spare.shape, 0)

    def close(a):
        for d in range(6):
            before, after = brims_ref[a, 0, d : d + 1], brims_ref[a, 1, d : d + 1]
            before = jnp.where(slab == 0, 0.0, before)
            after = jnp.where(slab == slabs - 1, 0.0, after)
            padded_ref[a, d, pl.ds(leaves, slots - leaves)] = jnp.where(
                at == 0, before, jnp.where(at == 1, after, spare)
            )

    for copy in copies[:2]:
        copy.wait()
    close(1)
    prepare(1)
    run((1,), True, 4)
    offsets = far_offsets()
    for q, around in enumerate(offsets):
        send(coefs_ref, windows_ref.at[q, pl.ds(8, leaves)], -around, 0)
        send(coefs_ref.at[pl.ds(leaves - 8, 8)], windows_ref.at[q, pl.ds(0, 8)], -around, 1)
        send(coefs_ref.at[pl.ds(0, 8)], windows_ref.at[q, pl.ds(leaves + 8, 8)], -around, -1)
    lax.fori_loop(0, distant * slabs, share_start, 0)
    for copy in copies[2:8]:
        copy.wait()
    close(0)
    close(2)
    prepare(0)
    prepare(2)
    run((0, 2), False, 2)
    for copy in copies[8:]:
        copy.wait()
    lax.fori_loop(0, distant * slabs, share_wait, 0)

    @pl.when(slab == 0)
    def _():
        windows_ref[:, pl.ds(0, 8)] = jnp.zeros_like(windows_ref[:, pl.ds(0, 8)])

    @pl.when(slab == slabs - 1)
    def _():
        windows_ref[:, pl.ds(leaves + 8, 8)] = jnp.zeros_like(windows_ref[:, pl.ds(0, 8)])

    total = None
    for q in range(len(offsets)):
        left, right = [], []
        for b in range(3):
            window = windows_ref[q, pl.ds(7 + b, leaves)]
            left.append(
                jnp.concatenate([window[:, rank * r : rank * r + rank] for r in range(count)], 0)
            )
            right.append(coupling_ref[3 * q + b] * mask_ref[0, 3 * q + b].astype(jnp.float32))
        term = split_product(
            stack_halves(jnp.concatenate(left, 1)), jnp.concatenate(right, 1), True
        )
        total = term if total is None else total + term
    far_ref[pl.ds(0, count * leaves)] = jnp.concatenate(
        [fold(total), jnp.zeros((count * leaves, far_ref.shape[1] - rank), jnp.float32)], 1
    )

    def facing(k):
        other = lax.rem(sector + REACH + 1 + k, sectors)
        held = shares_ref[other, 0]
        for p in range(1, slabs):
            held = held + shares_ref[other, p]
        return held[:, :rank], top_ref[other] * listed_ref[0, other].astype(jnp.float32)

    def across(k, carry):
        held, block = facing(k)
        return carry + fold(split_product(stack_halves(held), block, True))

    sector_local = jnp.zeros((8, rank), jnp.float32)
    if distant <= 4:
        if distant > 0:
            pairs = [facing(k) for k in range(distant)]
            held, block = (jnp.concatenate(x, 1) for x in zip(*pairs))
            sector_local = fold(split_product(stack_halves(held), block, True))
    else:
        sector_local = lax.fori_loop(0, distant, across, sector_local)
    slab_local = fold(split_product(stack_halves(sector_local), slab_ref[...], True))
    slab_left = stack_halves(slab_local)

    def down(g, carry):
        first = pl.multiple_of(8 * g, 8)
        sides = [far_ref[pl.ds(pl.multiple_of(leaves * r + 8 * g, 8), 8)] for r in range(count)]
        blank = jnp.zeros((8 - count, rank), jnp.float32)
        drops = [fold(split_product(slab_left, transfer_ref[first + n], True)) for n in range(8)]
        lefts = [
            stack_halves(
                drops[n] + jnp.concatenate([x[n : n + 1, :rank] for x in sides] + [blank], 0)
            )
            for n in range(8)
        ]
        spreads = [fold(split_product(lefts[n], basis_ref[first + n], False)) for n in range(8)]
        for r in range(count):
            rows = jnp.concatenate([x[r : r + 1] for x in spreads], 0)
            out_ref[r, pl.ds(first, 8)] = out_ref[r, pl.ds(first, 8)] + rows
        return carry

    lax.fori_loop(0, leaves // 8, down, 0)


def exchange(arrays):
    sectors, slabs = lax.axis_size("blk"), lax.axis_size("along")
    count, leaves, size = arrays[0].shape
    rank = arrays[3].shape[1]
    width = -(-count * rank // 128) * 128
    lanes = -(-rank // 128) * 128
    slots = -(-(leaves + 2) // 16) * 16
    far = 2 * (REACH - 1)
    links = 8 + 3 * far
    pairs = (sectors - 2 * REACH - 1) * slabs
    hbm = pl.BlockSpec(memory_space=pltpu.HBM)
    return pl.pallas_call(
        exchange_kernel,
        out_shape=jax.ShapeDtypeStruct((count, leaves, size), jnp.float32),
        in_specs=[hbm] * len(arrays),
        out_specs=pl.BlockSpec(memory_space=pltpu.VMEM),
        scratch_shapes=[
            *[pltpu.VMEM(x.shape, x.dtype) for x in arrays[:8]],
            *[pltpu.SMEM(x.shape, x.dtype) for x in arrays[8:]],
            pltpu.VMEM((6, leaves, size), jnp.float32),
            pltpu.VMEM((2, 8, size), jnp.float32),
            pltpu.VMEM((3, 6, slots, size), jnp.float32),
            pltpu.VMEM((3, 2, 8, size), jnp.float32),
            pltpu.VMEM((leaves, width), jnp.float32),
            pltpu.VMEM((far, leaves + 16, width), jnp.float32),
            pltpu.VMEM((8, lanes), jnp.float32),
            pltpu.VMEM((sectors, slabs, 8, lanes), jnp.float32),
            pltpu.VMEM((count * leaves, lanes), jnp.float32),
            pltpu.SemaphoreType.DMA((links,)),
            pltpu.SemaphoreType.DMA((links,)),
            pltpu.SemaphoreType.DMA((pairs,)),
            pltpu.SemaphoreType.DMA((pairs,)),
            pltpu.SemaphoreType.DMA((len(arrays),)),
            pltpu.VMEM((3, slots // 16, size, 256), jnp.bfloat16),
            pltpu.VMEM((slots * 16, 128), jnp.float32),
            pltpu.VMEM((slots * 16, 128), jnp.float32),
            pltpu.VMEM((3, slots * 16, size), jnp.bfloat16),
            pltpu.VMEM((10, leaves, size), jnp.float32),
            pltpu.VMEM((3, leaves, size), jnp.float32),
            *[pltpu.VMEM((12, size, size), jnp.bfloat16)] * 4,
        ],
        compiler_params=pltpu.CompilerParams(
            collective_id=0, has_side_effects=True, vmem_limit_bytes=40 * 1024 * 1024
        ),
    )(*arrays)


def body(
    values,
    offsets,
    stiffness,
    leaf_basis,
    transfer,
    slab_transfer_matrices,
    leaf_coupling_matrices,
    leaf_admissible_mask,
    top_coupling,
    top_admissible,
):
    arrays = (
        values[:, 0],
        offsets[:, 0],
        stiffness[0],
        leaf_basis[0],
        transfer[0],
        slab_transfer_matrices[0, 0],
        leaf_coupling_matrices[0],
        top_coupling[0],
        leaf_admissible_mask,
        top_admissible,
    )
    arrays = tuple(pltpu.with_memory_space_constraint(x, pltpu.HBM) for x in arrays)
    return exchange(arrays)[:, None]


def solution(mesh):
    return jax.shard_map(
        body,
        mesh=mesh,
        in_specs=(
            P(None, "blk", "along", None),
            P(None, "blk", "along", None),
            P("blk", "along", None),
            P("blk", "along", None, None),
            P("blk", "along", None, None),
            P("blk", "along", None, None),
            P("blk", None, None, None),
            P("blk", None),
            P("blk", None, None, None),
            P("blk", None),
        ),
        out_specs=P(None, "blk", "along", None),
        check_vma=False,
    )
```
